128 devices in a mesh: tp: 2 (over core), sp: 64 (over z, y, x).
Axes of the slice: x: 4, y: 4, z: 4, core: 2. Of those that a mesh axis runs over, the one named last changes fastest.
Arguments:
- x_tok: bfloat16 [96, 3072], replicated
- seq_lens: int32 [96], replicated
- k_cache: bfloat16 [96, 1024, 8, 128], P(None, 'sp', 'tp')
- v_cache: bfloat16 [96, 1024, 8, 128], P(None, 'sp', 'tp')
- g_attn: bfloat16 [3072], replicated
- w_q: bfloat16 [3072, 3072], P(None, 'tp')
- w_k: bfloat16 [3072, 1024], P(None, 'tp')
- w_v: bfloat16 [3072, 1024], P(None, 'tp')
- w_o: bfloat16 [3072, 3072], P('tp')
- g_mlp: bfloat16 [3072], replicated
- w_gate: bfloat16 [3072, 8192], P(None, 'tp')
- w_up: bfloat16 [3072, 8192], P(None, 'tp')
- w_down: bfloat16 [8192, 3072], P('tp')
Outputs:
- output 1: bfloat16 [96, 3072], replicated
- output 2: bfloat16 [96, 1024, 8, 128], P(None, 'sp', 'tp')
- output 3: bfloat16 [96, 1024, 8, 128], P(None, 'sp', 'tp')
All inputs are finite; a program needn't handle non-finite values.
Results may differ from the reference program's by a relative error of at most 0.0137389.
Values sent between devices are 32-bit elements.
A program may use at most 1 GiB of HBM per device.

```python
import math
import jax
import jax.numpy as jnp
from jax import lax

MODEL_DIM = 3072
Q_HEADS = 24
KV_HEADS = 8
HEAD_DIM = 128
FF_DIM = 8192
BATCH_SIZE = 96
SEQ_LEN = 1024

ROPE_BASE = 500000.0
NORM_EPS = 1e-5


def gauss_draw(rng_key, arr_shape):
    return jax.random.normal(rng_key, arr_shape, jnp.float32)


def draw_lens(rng_key):
    low_len = SEQ_LEN // 4
    key_len, key_hi, key_lo = jax.random.split(rng_key, 3)
    lens_raw = jax.random.randint(key_len, (BATCH_SIZE,), low_len, SEQ_LEN)
    idx_hi = jax.random.randint(key_hi, (), 0, BATCH_SIZE)
    idx_lo = (idx_hi + jax.random.randint(key_lo, (), 1, BATCH_SIZE)) % BATCH_SIZE
    row_ids = jnp.arange(BATCH_SIZE)
    lens_raw = jnp.where(row_ids == idx_hi, SEQ_LEN - 1, lens_raw)
    lens_raw = jnp.where(row_ids == idx_lo, low_len, lens_raw)
    return lens_raw.astype(jnp.int32)


def setup_inputs(seed: int = 0) -> dict:
    key_list = jax.random.split(jax.random.key(seed), 14)
    q_width = Q_HEADS * HEAD_DIM
    kv_width = KV_HEADS * HEAD_DIM
    groups = Q_HEADS // KV_HEADS
    cache_shape = (BATCH_SIZE, SEQ_LEN, KV_HEADS, HEAD_DIM)
    w_q32 = gauss_draw(key_list[4], (MODEL_DIM, q_width)) * MODEL_DIM ** -0.5
    self_gain = (math.log(SEQ_LEN) - 0.6) * math.sqrt(groups / HEAD_DIM)
    group_sum = jnp.sum(w_q32.reshape(MODEL_DIM, KV_HEADS, groups, HEAD_DIM), axis=2).reshape(MODEL_DIM, kv_width)
    w_k32 = group_sum * (self_gain / math.sqrt(groups)) + gauss_draw(key_list[5], (MODEL_DIM, kv_width)) * (0.5 * MODEL_DIM ** -0.5)
    value_scale = 0.5 * math.sqrt(SEQ_LEN)
    return {
        "x_tok": gauss_draw(key_list[0], (BATCH_SIZE, MODEL_DIM)).astype(jnp.bfloat16),
        "seq_lens": draw_lens(key_list[1]),
        "k_cache": gauss_draw(key_list[2], cache_shape).astype(jnp.bfloat16),
        "v_cache": (gauss_draw(key_list[3], cache_shape) * value_scale).astype(jnp.bfloat16),
        "g_attn": (1.0 + 0.2 * gauss_draw(key_list[6], (MODEL_DIM,))).astype(jnp.bfloat16),
        "w_q": w_q32.astype(jnp.bfloat16),
        "w_k": w_k32.astype(jnp.bfloat16),
        "w_v": (gauss_draw(key_list[7], (MODEL_DIM, kv_width)) * MODEL_DIM ** -0.5).astype(jnp.bfloat16),
        "w_o": (gauss_draw(key_list[8], (q_width, MODEL_DIM)) * q_width ** -0.5).astype(jnp.bfloat16),
        "g_mlp": (1.0 + 0.2 * gauss_draw(key_list[9], (MODEL_DIM,))).astype(jnp.bfloat16),
        "w_gate": (gauss_draw(key_list[10], (MODEL_DIM, FF_DIM)) * MODEL_DIM ** -0.5).astype(jnp.bfloat16),
        "w_up": (gauss_draw(key_list[11], (MODEL_DIM, FF_DIM)) * MODEL_DIM ** -0.5).astype(jnp.bfloat16),
        "w_down": (gauss_draw(key_list[12], (FF_DIM, MODEL_DIM)) * FF_DIM ** -0.5).astype(jnp.bfloat16),
    }


def rms_norm(x_in, norm_gain):
    x_f32 = x_in.astype(jnp.float32)
    inv_rms = lax.rsqrt(jnp.mean(x_f32 * x_f32, axis=-1, keepdims=True) + NORM_EPS)
    return (x_f32 * inv_rms * norm_gain.astype(jnp.float32)).astype(jnp.bfloat16)


def apply_rope(heads_in, positions):
    head_dim = heads_in.shape[-1]
    half_dim = head_dim // 2
    inv_freq = jnp.power(jnp.float32(ROPE_BASE), jnp.arange(half_dim, dtype=jnp.float32) * (-2.0 / head_dim))
    angles = positions.astype(jnp.float32)[:, None, None] * inv_freq
    cos_a = jnp.cos(angles)
    sin_a = jnp.sin(angles)
    heads_f32 = heads_in.astype(jnp.float32)
    first_half = heads_f32[..., :half_dim]
    second_half = heads_f32[..., half_dim:]
    rotated = jnp.concatenate([first_half * cos_a - second_half * sin_a, second_half * cos_a + first_half * sin_a], axis=-1)
    return rotated.astype(jnp.bfloat16)


def reference(x_tok, seq_lens, k_cache, v_cache, g_attn, w_q, w_k, w_v, w_o, g_mlp, w_gate, w_up, w_down):
    groups = Q_HEADS // KV_HEADS
    x_norm = rms_norm(x_tok, g_attn)
    q_new = jnp.dot(x_norm, w_q, preferred_element_type=jnp.float32).astype(jnp.bfloat16).reshape(BATCH_SIZE, Q_HEADS, HEAD_DIM)
    k_new = jnp.dot(x_norm, w_k, preferred_element_type=jnp.float32).astype(jnp.bfloat16).reshape(BATCH_SIZE, KV_HEADS, HEAD_DIM)
    v_new = jnp.dot(x_norm, w_v, preferred_element_type=jnp.float32).astype(jnp.bfloat16).reshape(BATCH_SIZE, KV_HEADS, HEAD_DIM)
    q_rot = apply_rope(q_new, seq_lens)
    k_rot = apply_rope(k_new, seq_lens)
    row_ids = jnp.arange(BATCH_SIZE)
    k_out = k_cache.at[row_ids, seq_lens].set(k_rot)
    v_out = v_cache.at[row_ids, seq_lens].set(v_new)
    score_scale = HEAD_DIM ** -0.5

    def attend_row(row_inputs):
        q_row, k_rows, v_rows, row_len = row_inputs
        scores = jnp.einsum("kgd,tkd->kgt", q_row.astype(jnp.float32), k_rows.astype(jnp.float32)) * score_scale
        is_valid = jnp.arange(SEQ_LEN) <= row_len
        masked = jnp.where(is_valid, scores, -jnp.inf)
        row_max = jnp.max(masked, axis=-1, keepdims=True)
        weights = jnp.exp(masked - row_max)
        row_sum = jnp.sum(weights, axis=-1, keepdims=True)
        mixed = jnp.einsum("kgt,tkd->kgd", weights.astype(jnp.bfloat16).astype(jnp.float32), v_rows.astype(jnp.float32))
        return (mixed / row_sum).astype(jnp.bfloat16)

    attn_heads = lax.map(attend_row, (q_rot.reshape(BATCH_SIZE, KV_HEADS, groups, HEAD_DIM), k_out, v_out, seq_lens))
    attn_flat = attn_heads.reshape(BATCH_SIZE, Q_HEADS * HEAD_DIM)
    attn_proj = jnp.dot(attn_flat, w_o, preferred_element_type=jnp.float32)
    hidden = (x_tok.astype(jnp.float32) + attn_proj).astype(jnp.bfloat16)
    h_norm = rms_norm(hidden, g_mlp)
    gate_proj = jnp.dot(h_norm, w_gate, preferred_element_type=jnp.float32).astype(jnp.bfloat16)
    up_proj = jnp.dot(h_norm, w_up, preferred_element_type=jnp.float32).astype(jnp.bfloat16)
    act_prod = (jax.nn.silu(gate_proj.astype(jnp.float32)) * up_proj.astype(jnp.float32)).astype(jnp.bfloat16)
    mlp_out = jnp.dot(act_prod, w_down, preferred_element_type=jnp.float32)
    y_out = (hidden.astype(jnp.float32) + mlp_out).astype(jnp.bfloat16)
    return (y_out, k_out, v_out)
```

```python
import jax
import jax.numpy as jnp
from jax import lax
from jax.experimental import pallas as pl
from jax.experimental.pallas import tpu as pltpu
from jax.sharding import PartitionSpec as P

ROPE_BASE = 500000.0
NORM_EPS = 1e-5


N_SP = 64
N_OWN = 48
MSG = 26

def sp_id(t):
    return {"sp": t}

def combine_kernel(send_ref, out_ref, recv, mine, gath, fac, send_sem, recv_sem, gsend_sem, grecv_sem):
    me = lax.axis_index("sp")
    barrier = pltpu.get_barrier_semaphore()

    @pl.loop(1, N_SP)
    def _(j):
        pl.semaphore_signal(barrier, inc=1, device_id=sp_id(lax.rem(me + j, N_SP)), device_id_type=pl.DeviceIdType.MESH)
    pl.semaphore_wait(barrier, N_SP - 1)

    @pl.loop(1, N_SP)
    def _(j):
        t = lax.rem(me + j, N_SP)
        @pl.when(t < N_OWN)
        def _():
            pltpu.make_async_remote_copy(src_ref=send_ref.at[t], dst_ref=recv.at[me], send_sem=send_sem, recv_sem=recv_sem,
                device_id=sp_id(t), device_id_type=pl.DeviceIdType.MESH).start()

    @pl.when(me < N_OWN)
    def _():
        recv[me] = send_ref[me]
        pltpu.make_async_copy(recv.at[pl.ds(0, N_SP - 1)], recv.at[pl.ds(0, N_SP - 1)], recv_sem).wait()
        m = recv[:, 24, :]
        l = recv[:, 25, :]
        top = jnp.max(m, axis=0, keepdims=True)
        f = jnp.exp(m - top)
        tot = jnp.sum(f * l, axis=0, keepdims=True)
        fac[...] = jnp.transpose(jnp.concatenate([f / tot, jnp.zeros((64, 128), jnp.float32)], axis=0))
        base = pl.multiple_of(lax.div(me, 12) * 24, 8)
        ft = fac[pl.ds(base, 24), :]
        acc = jnp.zeros((24, 128), jnp.float32)
        for i in range(N_SP):
            acc = acc + recv[i, 0:24, :] * ft[:, i:i + 1]
        mine[...] = acc.astype(jnp.bfloat16).astype(jnp.float32)
        gath[me] = mine[...]

        @pl.loop(1, N_SP)
        def _(j):
            t = lax.rem(me + j, N_SP)
            pltpu.make_async_remote_copy(src_ref=mine, dst_ref=gath.at[me], send_sem=gsend_sem, recv_sem=grecv_sem,
                device_id=sp_id(t), device_id_type=pl.DeviceIdType.MESH).start()
        pltpu.make_async_copy(gath.at[pl.ds(0, N_OWN - 1)], gath.at[pl.ds(0, N_OWN - 1)], grecv_sem).wait()
        pltpu.make_async_copy(send_ref.at[pl.ds(0, N_OWN - 1)], send_ref.at[pl.ds(0, N_OWN - 1)], send_sem).wait()
        @pl.loop(1, N_SP)
        def _(j):
            pltpu.make_async_copy(mine, mine, gsend_sem).wait()

    @pl.when(me >= N_OWN)
    def _():
        pltpu.make_async_copy(gath, gath, grecv_sem).wait()
        pltpu.make_async_copy(send_ref, send_ref, send_sem).wait()

    for kv in range(4):
        for g in range(3):
            h = kv * 3 + g
            out_ref[:, h * 128:(h + 1) * 128] = gath[kv * 12:(kv + 1) * 12, g * 8:(g + 1) * 8, :].reshape(96, 128).astype(jnp.bfloat16)


def combine(send):
    return pl.pallas_call(
        combine_kernel,
        out_shape=jax.ShapeDtypeStruct((96, 1536), jnp.bfloat16),
        in_specs=[pl.BlockSpec(memory_space=pltpu.VMEM)],
        out_specs=pl.BlockSpec(memory_space=pltpu.VMEM),
        scratch_shapes=[
            pltpu.VMEM((N_SP, MSG, 128), jnp.float32),
            pltpu.VMEM((24, 128), jnp.float32),
            pltpu.VMEM((N_OWN, 24, 128), jnp.float32),
            pltpu.VMEM((128, 128), jnp.float32),
            pltpu.SemaphoreType.DMA, pltpu.SemaphoreType.DMA, pltpu.SemaphoreType.DMA, pltpu.SemaphoreType.DMA,
        ],
        compiler_params=pltpu.CompilerParams(collective_id=1, has_side_effects=True),
        name="combine",
    )(send)


def rms_norm(x_in, norm_gain):
    x_f32 = x_in.astype(jnp.float32)
    inv_rms = lax.rsqrt(jnp.mean(x_f32 * x_f32, axis=-1, keepdims=True) + NORM_EPS)
    return (x_f32 * inv_rms * norm_gain.astype(jnp.float32)).astype(jnp.bfloat16)


def apply_rope(heads_in, positions):
    head_dim = heads_in.shape[-1]
    half_dim = head_dim // 2
    inv_freq = jnp.power(jnp.float32(ROPE_BASE), jnp.arange(half_dim, dtype=jnp.float32) * (-2.0 / head_dim))
    angles = positions.astype(jnp.float32)[:, None, None] * inv_freq
    cos_a = jnp.cos(angles)
    sin_a = jnp.sin(angles)
    heads_f32 = heads_in.astype(jnp.float32)
    first_half = heads_f32[..., :half_dim]
    second_half = heads_f32[..., half_dim:]
    rotated = jnp.concatenate([first_half * cos_a - second_half * sin_a, second_half * cos_a + first_half * sin_a], axis=-1)
    return rotated.astype(jnp.bfloat16)


def solution(mesh):
    cache_spec = P(None, "sp", "tp", None)
    col_spec = P(None, "tp")
    row_spec = P("tp", None)
    full_spec = P()

    def local_step(x_tok, seq_lens, k_blk, v_blk, g_attn, wq_loc, wk_loc, wv_loc, wo_loc, g_mlp, wg_loc, wu_loc, wd_loc):
        batch_rows, seq_blk, kv_loc, head_dim = k_blk.shape
        q_loc = wq_loc.shape[1] // head_dim
        groups = q_loc // kv_loc
        x_norm = rms_norm(x_tok, g_attn)
        q_new = jnp.dot(x_norm, wq_loc, preferred_element_type=jnp.float32).astype(jnp.bfloat16).reshape(batch_rows, q_loc, head_dim)
        k_new = jnp.dot(x_norm, wk_loc, preferred_element_type=jnp.float32).astype(jnp.bfloat16).reshape(batch_rows, kv_loc, head_dim)
        v_new = jnp.dot(x_norm, wv_loc, preferred_element_type=jnp.float32).astype(jnp.bfloat16).reshape(batch_rows, kv_loc, head_dim)
        q_rot = apply_rope(q_new, seq_lens)
        k_rot = apply_rope(k_new, seq_lens)
        local_pos = lax.axis_index("sp") * seq_blk + jnp.arange(seq_blk)
        is_new = (local_pos[None, :] == seq_lens[:, None])[:, :, None, None]
        k_out = jnp.where(is_new, k_rot[:, None], k_blk)
        v_out = jnp.where(is_new, v_new[:, None], v_blk)
        q_grp = q_rot.reshape(batch_rows, kv_loc, groups, head_dim)
        scores = jnp.einsum("bkgd,bskd->bkgs", q_grp, k_out, preferred_element_type=jnp.float32) * (head_dim ** -0.5)
        is_valid = (local_pos[None, :] <= seq_lens[:, None])[:, None, None, :]
        masked = jnp.where(is_valid, scores, -1e30)
        blk_max = jnp.max(masked, axis=-1, keepdims=True)
        weights = jnp.where(is_valid, jnp.exp(masked - blk_max), 0.0)
        blk_sum = jnp.sum(weights, axis=-1, keepdims=True)
        blk_mix = jnp.einsum("bkgs,bskd->bkgd", weights.astype(jnp.bfloat16), v_out, preferred_element_type=jnp.float32)
        mix_rows = blk_mix.reshape(12, 8, kv_loc, groups, head_dim).transpose(2, 0, 3, 1, 4).reshape(48, 24, head_dim)

        def stat_rows(stat):
            lanes = stat.reshape(12, 8, kv_loc * groups).transpose(0, 2, 1).reshape(12, 1, 96)
            return jnp.broadcast_to(jnp.pad(lanes, ((0, 0), (0, 0), (0, 32)))[None], (kv_loc, 12, 1, 128)).reshape(48, 1, 128)

        send = jnp.concatenate([mix_rows, stat_rows(blk_max), stat_rows(blk_sum)], axis=1)
        attn_out = combine(send)
        attn_proj = lax.psum(jnp.dot(attn_out, wo_loc, preferred_element_type=jnp.float32), "tp")
        hidden = (x_tok.astype(jnp.float32) + attn_proj).astype(jnp.bfloat16)
        h_norm = rms_norm(hidden, g_mlp)
        gate_proj = jnp.dot(h_norm, wg_loc, preferred_element_type=jnp.float32).astype(jnp.bfloat16)
        up_proj = jnp.dot(h_norm, wu_loc, preferred_element_type=jnp.float32).astype(jnp.bfloat16)
        act_prod = (jax.nn.silu(gate_proj.astype(jnp.float32)) * up_proj.astype(jnp.float32)).astype(jnp.bfloat16)
        mlp_out = lax.psum(jnp.dot(act_prod, wd_loc, preferred_element_type=jnp.float32), "tp")
        y_out = (hidden.astype(jnp.float32) + mlp_out).astype(jnp.bfloat16)
        return y_out, k_out, v_out

    return jax.shard_map(local_step, mesh=mesh, in_specs=(full_spec, full_spec, cache_spec, cache_spec, full_spec, col_spec, col_spec, col_spec, row_spec, full_spec, col_spec, col_spec, row_spec), out_specs=(full_spec, cache_spec, cache_spec), check_vma=False)
```

```python
import jax
import jax.numpy as jnp
from jax import lax
from jax.experimental import pallas as pl
from jax.experimental.pallas import tpu as pltpu
from jax.sharding import PartitionSpec as P

ROPE_BASE = 500000.0
NORM_EPS = 1e-5
N_SP = 64
N_OWN = 48
MSG = 26
SLOTS = 16
MESH = pl.DeviceIdType.MESH


def rest_kernel(send_ref, x_ref, g_ref, wo, wg, wu, wd, y_ref,
                recv, mine, gath, fac, attn, part, prem, hid, z_scr, act, wbuf,
                send_sem, recv_sem, gsend_sem, grecv_sem, psend_sem, precv_sem, wsem):
    me = lax.axis_index("sp")
    tp = lax.axis_index("tp")
    barrier = pltpu.get_barrier_semaphore()

    @pl.loop(1, N_SP)
    def _(j):
        pl.semaphore_signal(barrier, inc=1, device_id={"sp": lax.rem(me + j, N_SP)}, device_id_type=MESH)
    pl.semaphore_signal(barrier, inc=1, device_id={"tp": 1 - tp}, device_id_type=MESH)

    def cols(c):
        return pl.ds(pl.multiple_of(c * 512, 512), 512)

    def load(src, slot, rows):
        return pltpu.make_async_copy(src, wbuf.at[slot, rows], wsem.at[slot])

    def start_wo(j):
        for half in range(2):
            load(wo.at[:, pl.ds((2 * j + half) * 512, 512)], j, pl.ds(half * 1536, 1536)).start()

    def start_gu(c):
        load(wg.at[:, cols(c)], lax.rem(3 + 2 * c, SLOTS), pl.ds(0, 3072)).start()
        load(wu.at[:, cols(c)], lax.rem(4 + 2 * c, SLOTS), pl.ds(0, 3072)).start()

    def start_wd(m):
        for third in range(3):
            piece = 3 * m + third
            n, kq = lax.div(piece, 4), lax.rem(piece, 4)
            load(wd.at[pl.ds(pl.multiple_of(kq * 1024, 1024), 1024), cols(n)], lax.rem(3 + m, SLOTS), pl.ds(third * 1024, 1024)).start()

    def arrived(slot):
        pltpu.make_async_copy(wbuf.at[slot], wbuf.at[slot], wsem.at[slot]).wait()

    for j in range(3):
        start_wo(j)

    @pl.loop(0, 6)
    def _(c):
        start_gu(c)
    load(wg.at[:, pl.ds(6 * 512, 512)], 15, pl.ds(0, 3072)).start()

    pl.semaphore_wait(barrier, N_SP)

    @pl.loop(1, N_SP)
    def _(j):
        t = lax.rem(me + j, N_SP)

        @pl.when(t < N_OWN)
        def _():
            pltpu.make_async_remote_copy(src_ref=send_ref.at[t], dst_ref=recv.at[me], send_sem=send_sem, recv_sem=recv_sem,
                                         device_id={"sp": t}, device_id_type=MESH).start()

    @pl.when(me < N_OWN)
    def _():
        recv[me] = send_ref[me]
        pltpu.make_async_copy(recv.at[pl.ds(0, N_SP - 1)], recv.at[pl.ds(0, N_SP - 1)], recv_sem).wait()
        top = jnp.max(recv[:, 24, :], axis=0, keepdims=True)
        f = jnp.exp(recv[:, 24, :] - top)
        tot = jnp.sum(f * recv[:, 25, :], axis=0, keepdims=True)
        fac[...] = jnp.transpose(jnp.concatenate([f, jnp.broadcast_to(tot, (64, 128))], axis=0))
        ft = fac[pl.ds(pl.multiple_of(lax.div(me, 12) * 24, 8), 24), :]
        acc = [jnp.zeros((24, 128), jnp.float32) for _ in range(4)]
        for i in range(N_SP):
            acc[i % 4] = acc[i % 4] + recv[i, 0:24, :] * ft[:, i:i + 1]
        total = (acc[0] + acc[1]) + (acc[2] + acc[3])
        mine[...] = (total / ft[:, 64:65]).astype(jnp.bfloat16).astype(jnp.float32)
        gath[me] = mine[...]

        @pl.loop(1, N_SP)
        def _(j):
            pltpu.make_async_remote_copy(src_ref=mine, dst_ref=gath.at[me], send_sem=gsend_sem, recv_sem=grecv_sem,
                                         device_id={"sp": lax.rem(me + j, N_SP)}, device_id_type=MESH).start()
        pltpu.make_async_copy(gath.at[pl.ds(0, N_OWN - 1)], gath.at[pl.ds(0, N_OWN - 1)], grecv_sem).wait()

    @pl.when(me >= N_OWN)
    def _():
        pltpu.make_async_copy(gath, gath, grecv_sem).wait()

    for kv in range(4):
        for g in range(3):
            h = kv * 3 + g
            attn[:, h * 128:(h + 1) * 128] = gath[kv * 12:(kv + 1) * 12, g * 8:(g + 1) * 8, :].reshape(96, 128).astype(jnp.bfloat16)

    def exchange(phase, n):
        return pltpu.make_async_remote_copy(src_ref=part.at[phase, n], dst_ref=prem.at[phase, n], send_sem=psend_sem.at[phase, n],
                                            recv_sem=precv_sem.at[phase, n], device_id={"tp": 1 - tp}, device_id_type=MESH)

    for j in range(3):
        arrived(j)
        for half in range(2):
            n = 2 * j + half
            part[0, n] = jnp.dot(attn[...], wbuf[j, half * 1536:(half + 1) * 1536, :], preferred_element_type=jnp.float32)
            exchange(0, n).start()
        if j == 0:
            load(wu.at[:, pl.ds(6 * 512, 512)], 0, pl.ds(0, 3072)).start()
        if j == 1:
            load(wg.at[:, pl.ds(7 * 512, 512)], 1, pl.ds(0, 3072)).start()
        if j == 2:
            load(wu.at[:, pl.ds(7 * 512, 512)], 2, pl.ds(0, 3072)).start()
    sq = jnp.zeros((96, 128), jnp.float32)
    for n in range(6):
        exchange(0, n).wait_recv()
        for q in range(4):
            at = slice(n * 512 + q * 128, n * 512 + (q + 1) * 128)
            here = slice(q * 128, (q + 1) * 128)
            h = (x_ref[:, at].astype(jnp.float32) + (part[0, n, :, here] + prem[0, n, :, here])).astype(jnp.bfloat16)
            hid[:, at] = h
            h = h.astype(jnp.float32)
            sq = sq + h * h
    inv = lax.rsqrt(jnp.sum(sq, axis=-1, keepdims=True) * (1.0 / 3072.0) + NORM_EPS)
    for c in range(24):
        at = slice(c * 128, (c + 1) * 128)
        z_scr[:, at] = (hid[:, at].astype(jnp.float32) * inv * g_ref[c:c + 1, :].astype(jnp.float32)).astype(jnp.bfloat16)

    @pl.loop(0, 8)
    def _(c):
        sg = lax.rem(3 + 2 * c, SLOTS)
        su = lax.rem(4 + 2 * c, SLOTS)
        arrived(sg)
        gate = jnp.dot(z_scr[...], wbuf[sg], preferred_element_type=jnp.float32).astype(jnp.bfloat16).astype(jnp.float32)
        arrived(su)
        up = jnp.dot(z_scr[...], wbuf[su], preferred_element_type=jnp.float32).astype(jnp.bfloat16).astype(jnp.float32)
        act[:, cols(c)] = (gate * lax.logistic(gate) * up).astype(jnp.bfloat16)

        @pl.when(c < 4)
        def _():
            start_wd(2 * c)
            start_wd(2 * c + 1)

    waited = -1
    for n in range(6):
        total = None
        for kq in range(4):
            m, third = divmod(n * 4 + kq, 3)
            if m > waited:
                arrived((3 + m) % SLOTS)
                waited = m
            d = jnp.dot(act[:, kq * 1024:(kq + 1) * 1024], wbuf[(3 + m) % SLOTS, third * 1024:(third + 1) * 1024, :], preferred_element_type=jnp.float32)
            total = d if total is None else total + d
        part[1, n] = total
        exchange(1, n).start()
    for n in range(6):
        exchange(1, n).wait_recv()
        at = slice(n * 512, (n + 1) * 512)
        y_ref[:, at] = (hid[:, at].astype(jnp.float32) + (part[1, n] + prem[1, n])).astype(jnp.bfloat16)

    for n in range(6):
        exchange(0, n).wait_send()
        exchange(1, n).wait_send()

    @pl.when(me < N_OWN)
    def _():
        pltpu.make_async_copy(send_ref.at[pl.ds(0, N_OWN - 1)], send_ref.at[pl.ds(0, N_OWN - 1)], send_sem).wait()

        @pl.loop(1, N_SP)
        def _(j):
            pltpu.make_async_copy(mine, mine, gsend_sem).wait()

    @pl.when(me >= N_OWN)
    def _():
        pltpu.make_async_copy(send_ref, send_ref, send_sem).wait()


def rest_part(send, x_tok, g_mlp, wo, wg, wu, wd):
    vmem = pl.BlockSpec(memory_space=pltpu.VMEM)
    hbm = pl.BlockSpec(memory_space=pl.ANY)
    f32, bf16 = jnp.float32, jnp.bfloat16
    return pl.pallas_call(
        rest_kernel,
        out_shape=jax.ShapeDtypeStruct((96, 3072), bf16),
        in_specs=[vmem, vmem, vmem, hbm, hbm, hbm, hbm],
        out_specs=vmem,
        scratch_shapes=[
            pltpu.VMEM((N_SP, MSG, 128), f32),
            pltpu.VMEM((24, 128), f32),
            pltpu.VMEM((N_OWN, 24, 128), f32),
            pltpu.VMEM((128, 128), f32),
            pltpu.VMEM((96, 1536), bf16),
            pltpu.VMEM((2, 6, 96, 512), f32),
            pltpu.VMEM((2, 6, 96, 512), f32),
            pltpu.VMEM((96, 3072), bf16),
            pltpu.VMEM((96, 3072), bf16),
            pltpu.VMEM((96, 4096), bf16),
            pltpu.VMEM((SLOTS, 3072, 512), bf16),
            pltpu.SemaphoreType.DMA, pltpu.SemaphoreType.DMA, pltpu.SemaphoreType.DMA, pltpu.SemaphoreType.DMA,
            pltpu.SemaphoreType.DMA((2, 6)), pltpu.SemaphoreType.DMA((2, 6)), pltpu.SemaphoreType.DMA((SLOTS,)),
        ],
        compiler_params=pltpu.CompilerParams(collective_id=1, has_side_effects=True, vmem_limit_bytes=67043328),
        cost_estimate=pl.CostEstimate(flops=2 * 96 * 42_500_000, bytes_accessed=90_000_000, transcendentals=400_000),
        name="rest_part",
    )(send, x_tok, g_mlp.reshape(24, 128), wo, wg, wu, wd)


def local_kernel(seq_ref, x_ref, g_ref, cos_ref, sin_ref, kin, vin, wq, wk, wv,
                 send_ref, kout, vout, wbuf, kbuf, vbuf, u_scr, q_scr, new_scr, wsem, csem, osem):
    sp = lax.axis_index("sp")
    chunks = [(wk, 0), (wv, 0), (wq, 0), (wq, 1), (wq, 2)]
    wcopies = [pltpu.make_async_copy(w.at[:, pl.ds(c * 512, 512)], wbuf.at[i], wsem.at[i]) for i, (w, c) in enumerate(chunks)]
    kcopy = pltpu.make_async_copy(kin, kbuf, csem.at[0])
    vcopy = pltpu.make_async_copy(vin, vbuf, csem.at[1])
    for copy in wcopies[:2] + [kcopy, vcopy] + wcopies[2:]:
        copy.start()

    sq = jnp.zeros((96, 128), jnp.float32)
    for c in range(24):
        xc = x_ref[:, c * 128:(c + 1) * 128].astype(jnp.float32)
        sq = sq + xc * xc
    inv = lax.rsqrt(jnp.sum(sq, axis=-1, keepdims=True) * (1.0 / 3072.0) + NORM_EPS)
    for c in range(24):
        xc = x_ref[:, c * 128:(c + 1) * 128].astype(jnp.float32)
        u_scr[:, c * 128:(c + 1) * 128] = (xc * inv * g_ref[c:c + 1, :].astype(jnp.float32)).astype(jnp.bfloat16)
    u = u_scr[...]
    cos_a = cos_ref[...]
    sin_a = sin_ref[...]

    def project(i):
        wcopies[i].wait()
        return jnp.dot(u, wbuf[i], preferred_element_type=jnp.float32).astype(jnp.bfloat16).astype(jnp.float32)

    def rope(h):
        return (h * cos_a + pltpu.roll(h, 64, 1) * sin_a).astype(jnp.bfloat16).astype(jnp.float32)

    rowpos = lax.broadcasted_iota(jnp.int32, (64, 128), 0) // 4 + sp * 16

    def update(i, cin, buf, turn, out, sem):
        fresh = project(i)
        for kv in range(4):
            rows = fresh[:, kv * 128:(kv + 1) * 128]
            rows = rope(rows) if turn else rows
            new_scr[pl.ds(kv, 96, stride=8), :] = rows
            new_scr[pl.ds(kv + 4, 96, stride=8), :] = rows
        cin.wait()

        @pl.loop(0, 12)
        def _(bg):
            for j in range(8):
                b = bg * 8 + j
                tile = new_scr[pl.ds(pl.multiple_of(b * 8, 8), 8), :]
                old = buf[b].astype(jnp.float32)
                wide = jnp.broadcast_to(tile[None], (8, 8, 128)).reshape(64, 128)
                buf[b] = jnp.where(rowpos == seq_ref[b], wide, old).astype(jnp.bfloat16)
        copy = pltpu.make_async_copy(buf, out, sem)
        copy.start()
        return copy

    ocopies = [update(0, kcopy, kbuf, True, kout, osem.at[0]), update(1, vcopy, vbuf, False, vout, osem.at[1])]

    for c in range(3):
        q = project(2 + c)
        for j in range(4):
            q_scr[:, c * 4 + j] = rope(q[:, j * 128:(j + 1) * 128]).reshape(12, 8, 128)

    col = lax.broadcasted_iota(jnp.int32, (8, 512), 1)
    sub = lax.broadcasted_iota(jnp.int32, (8, 512), 0)
    own_req = (col // 64) == sub
    colpos = (col % 64) // 4 + sp * 16
    diag = lax.broadcasted_iota(jnp.int32, (96, 128), 0) == lax.broadcasted_iota(jnp.int32, (96, 128), 1)

    @pl.loop(0, 12)
    def _(bg):
        q = q_scr[bg].reshape(96, 128).astype(jnp.bfloat16)
        k = kbuf[pl.ds(bg * 8, 8)].reshape(512, 128)
        v = vbuf[pl.ds(bg * 8, 8)].reshape(512, 128)
        s = lax.dot_general(q, k, (((1,), (1,)), ((), ())), preferred_element_type=jnp.float32) * (128.0 ** -0.5)
        last = jnp.zeros((8, 512), jnp.int32)
        for j in range(8):
            last = jnp.where(sub == j, seq_ref[bg * 8 + j], last)
        ok = own_req & (colpos <= last)
        weights, tops, sums = [], [], []
        for kv in range(4):
            seen = ok & ((col % 4) == kv)
            for g in range(3):
                h = kv * 3 + g
                masked = jnp.where(seen, s[h * 8:(h + 1) * 8, :], -1e30)
                top = jnp.max(masked, axis=-1, keepdims=True)
                w = jnp.where(seen, jnp.exp(masked - top), 0.0)
                weights.append(w)
                tops.append(jnp.broadcast_to(top, (8, 128)))
                sums.append(jnp.broadcast_to(jnp.sum(w, axis=-1, keepdims=True), (8, 128)))
        w = jnp.concatenate(weights, axis=0).astype(jnp.bfloat16)
        mix = jnp.dot(w, v, preferred_element_type=jnp.float32)
        top_row = jnp.sum(jnp.where(diag, jnp.concatenate(tops, axis=0), 0.0), axis=0, keepdims=True)
        sum_row = jnp.sum(jnp.where(diag, jnp.concatenate(sums, axis=0), 0.0), axis=0, keepdims=True)
        for kv in range(4):
            send_ref[kv * 12 + bg, 0:24, :] = mix[kv * 24:(kv + 1) * 24, :]
            send_ref[kv * 12 + bg, 24:25, :] = top_row
            send_ref[kv * 12 + bg, 25:26, :] = sum_row

    for copy in ocopies:
        copy.wait()


def local_part(seq_lens, x_tok, g_attn, k_blk, v_blk, wq, wk, wv):
    inv_freq = jnp.power(jnp.float32(ROPE_BASE), jnp.arange(64, dtype=jnp.float32) * (-2.0 / 128))
    angles = seq_lens.astype(jnp.float32)[:, None] * inv_freq
    cos_a, sin_a = jnp.cos(angles), jnp.sin(angles)
    cos2 = jnp.concatenate([cos_a, cos_a], axis=-1)
    sin2 = jnp.concatenate([-sin_a, sin_a], axis=-1)
    vmem = pl.BlockSpec(memory_space=pltpu.VMEM)
    hbm = pl.BlockSpec(memory_space=pl.ANY)
    cache = jax.ShapeDtypeStruct((96, 64, 128), jnp.bfloat16)
    send, k_out, v_out = pl.pallas_call(
        local_kernel,
        out_shape=(jax.ShapeDtypeStruct((48, MSG, 128), jnp.float32), cache, cache),
        in_specs=[pl.BlockSpec(memory_space=pltpu.SMEM), vmem, vmem, vmem, vmem, hbm, hbm, hbm, hbm, hbm],
        out_specs=(vmem, hbm, hbm),
        scratch_shapes=[
            pltpu.VMEM((5, 3072, 512), jnp.bfloat16),
            pltpu.VMEM((96, 64, 128), jnp.bfloat16),
            pltpu.VMEM((96, 64, 128), jnp.bfloat16),
            pltpu.VMEM((96, 3072), jnp.bfloat16),
            pltpu.VMEM((12, 12, 8, 128), jnp.float32),
            pltpu.VMEM((768, 128), jnp.float32),
            pltpu.SemaphoreType.DMA((5,)),
            pltpu.SemaphoreType.DMA((2,)),
            pltpu.SemaphoreType.DMA((2,)),
        ],
        compiler_params=pltpu.CompilerParams(vmem_limit_bytes=67043328),
        cost_estimate=pl.CostEstimate(flops=2 * 96 * 3072 * 2560, bytes_accessed=22_000_000, transcendentals=600_000),
        name="local_part",
    )(seq_lens, x_tok, g_attn.reshape(24, 128), cos2, sin2, k_blk.reshape(96, 64, 128), v_blk.reshape(96, 64, 128), wq, wk, wv)
    return send, k_out.reshape(k_blk.shape), v_out.reshape(v_blk.shape)


def solution(mesh):
    cache_spec = P(None, "sp", "tp", None)
    col_spec = P(None, "tp")
    row_spec = P("tp", None)
    full_spec = P()

    def local_step(x_tok, seq_lens, k_blk, v_blk, g_attn, wq_loc, wk_loc, wv_loc, wo_loc, g_mlp, wg_loc, wu_loc, wd_loc):
        send, k_out, v_out = local_part(seq_lens, x_tok, g_attn, k_blk, v_blk, wq_loc, wk_loc, wv_loc)
        y_out = rest_part(send, x_tok, g_mlp, wo_loc, wg_loc, wu_loc, wd_loc)
        return y_out, k_out, v_out

    return jax.shard_map(local_step, mesh=mesh, in_specs=(full_spec, full_spec, cache_spec, cache_spec, full_spec, col_spec, col_spec, col_spec, row_spec, full_spec, col_spec, col_spec, row_spec), out_specs=(full_spec, cache_spec, cache_spec), check_vma=False)
```

```python
import jax
import jax.numpy as jnp
import numpy as np
from jax import lax
from jax.experimental import pallas as pl
from jax.experimental.pallas import tpu as pltpu
from jax.sharding import PartitionSpec as P

ROPE_BASE = 500000.0
NORM_EPS = 1e-5
N_SP = 64
N_OWN = 48
MSG = 26
SLOTS = 16
MESH = pl.DeviceIdType.MESH


def norm_into(x_ref, g_ref, out_ref):
    sq = jnp.zeros((96, 128), jnp.float32)
    for c in range(24):
        xc = x_ref[:, c * 128:(c + 1) * 128].astype(jnp.float32)
        sq = sq + xc * xc
    inv = lax.rsqrt(jnp.sum(sq, axis=-1, keepdims=True) * (1.0 / 3072.0) + NORM_EPS)
    for c in range(24):
        xc = x_ref[:, c * 128:(c + 1) * 128].astype(jnp.float32)
        out_ref[:, c * 128:(c + 1) * 128] = (xc * inv * g_ref[c:c + 1, :].astype(jnp.float32)).astype(jnp.bfloat16)


def rope(h, cos_a, sin_a):
    return (h * cos_a + pltpu.roll(h, 64, 1) * sin_a).astype(jnp.bfloat16).astype(jnp.float32)


def cache_kernel(seq_ref, x_ref, g_ref, freq_ref, kin, vin, wk, wv, kout, vout, cos_ref, sin_ref,
                 wbuf, kbuf, vbuf, u_scr, new_scr, wsem, csem, osem):
    sp = lax.axis_index("sp")
    wcopies = [pltpu.make_async_copy(w, wbuf.at[i], wsem.at[i]) for i, w in enumerate((wk, wv))]
    ccopies = [pltpu.make_async_copy(kin, kbuf, csem.at[0]), pltpu.make_async_copy(vin, vbuf, csem.at[1])]
    for copy in (wcopies[0], ccopies[0], wcopies[1], ccopies[1]):
        copy.start()
    norm_into(x_ref, g_ref, u_scr)
    u = u_scr[...]

    sub = lax.broadcasted_iota(jnp.int32, (8, 128), 0)
    low = lax.broadcasted_iota(jnp.int32, (8, 128), 1) < 64
    for bg in range(12):
        pos = jnp.zeros((8, 128), jnp.int32)
        for j in range(8):
            pos = jnp.where(sub == j, seq_ref[bg * 8 + j], pos)
        angle = pos.astype(jnp.float32) * freq_ref[...]
        cos_ref[bg * 8:(bg + 1) * 8, :] = jnp.cos(angle)
        sin_a = jnp.sin(angle)
        sin_ref[bg * 8:(bg + 1) * 8, :] = jnp.where(low, -sin_a, sin_a)

    rowpos = lax.broadcasted_iota(jnp.int32, (64, 128), 0) // 4 + sp * 16

    def update(i, buf, turn, out):
        wcopies[i].wait()
        fresh = jnp.dot(u, wbuf[i], preferred_element_type=jnp.float32).astype(jnp.bfloat16).astype(jnp.float32)
        for kv in range(4):
            rows = fresh[:, kv * 128:(kv + 1) * 128]
            rows = rope(rows, cos_ref[...], sin_ref[...]) if turn else rows
            new_scr[pl.ds(kv, 96, stride=8), :] = rows
            new_scr[pl.ds(kv + 4, 96, stride=8), :] = rows
        ccopies[i].wait()

        @pl.loop(0, 12)
        def _(bg):
            for j in range(8):
                b = bg * 8 + j
                tile = new_scr[pl.ds(pl.multiple_of(b * 8, 8), 8), :]
                wide = jnp.broadcast_to(tile[None], (8, 8, 128)).reshape(64, 128)
                buf[b] = jnp.where(rowpos == seq_ref[b], wide, buf[b].astype(jnp.float32)).astype(jnp.bfloat16)
            pltpu.make_async_copy(buf.at[pl.ds(bg * 8, 8)], out.at[pl.ds(bg * 8, 8)], osem.at[i]).start()

    update(0, kbuf, True, kout)
    update(1, vbuf, False, vout)
    pltpu.make_async_copy(kbuf, kout, osem.at[0]).wait()
    pltpu.make_async_copy(vbuf, vout, osem.at[1]).wait()


def cache_part(seq_lens, x_tok, g_attn, k_blk, v_blk, wk, wv):
    inv_freq = np.power(ROPE_BASE, np.arange(64) * (-2.0 / 128)).astype(np.float32)
    freq = jnp.asarray(np.tile(inv_freq, (8, 2)))
    vmem = pl.BlockSpec(memory_space=pltpu.VMEM)
    hbm = pl.BlockSpec(memory_space=pl.ANY)
    cache = jax.ShapeDtypeStruct((96, 64, 128), jnp.bfloat16)
    table = jax.ShapeDtypeStruct((96, 128), jnp.float32)
    return pl.pallas_call(
        cache_kernel,
        out_shape=(cache, cache, table, table),
        in_specs=[pl.BlockSpec(memory_space=pltpu.SMEM), vmem, vmem, vmem, hbm, hbm, hbm, hbm],
        out_specs=(hbm, hbm, vmem, vmem),
        scratch_shapes=[
            pltpu.VMEM((2, 3072, 512), jnp.bfloat16),
            pltpu.VMEM((96, 64, 128), jnp.bfloat16),
            pltpu.VMEM((96, 64, 128), jnp.bfloat16),
            pltpu.VMEM((96, 3072), jnp.bfloat16),
            pltpu.VMEM((768, 128), jnp.float32),
            pltpu.SemaphoreType.DMA((2,)), pltpu.SemaphoreType.DMA((2,)), pltpu.SemaphoreType.DMA((2,)),
        ],
        compiler_params=pltpu.CompilerParams(vmem_limit_bytes=67043328),
        cost_estimate=pl.CostEstimate(flops=2 * 96 * 3072 * 1024, bytes_accessed=13_000_000, transcendentals=30_000),
        name="cache_part",
    )(seq_lens, x_tok, g_attn.reshape(24, 128), freq, k_blk.reshape(96, 64, 128), v_blk.reshape(96, 64, 128), wk, wv)


def main_kernel(seq_ref, x_ref, g1_ref, g2_ref, cos_ref, sin_ref, kout, vout, wq, wo, wg, wu, wd, y_ref,
                send, recv, mine, gath, fac, part, prem, u_scr, wbuf,
                send_sem, recv_sem, gsend_sem, grecv_sem, psend_sem, precv_sem, wsem, csem):
    me = lax.axis_index("sp")
    tp = lax.axis_index("tp")
    barrier = pltpu.get_barrier_semaphore()

    def turn_of(t):
        return lax.rem(lax.rem(t, 4) + lax.rem(lax.div(t, 4), 4) + lax.div(t, 16), 4)

    owner = turn_of(me) < 3
    my_own = lax.div(me, 4) * 3 + turn_of(me)

    def device_of(o):
        yz = lax.div(o, 3)
        return yz * 4 + lax.rem(lax.rem(o, 3) + 8 - lax.rem(yz, 4) - lax.div(yz, 4), 4)

    @pl.loop(1, N_SP)
    def _(j):
        pl.semaphore_signal(barrier, inc=1, device_id={"sp": lax.rem(me + j, N_SP)}, device_id_type=MESH)
    pl.semaphore_signal(barrier, inc=1, device_id={"tp": 1 - tp}, device_id_type=MESH)

    def cols(c):
        return pl.ds(pl.multiple_of(c * 512, 512), 512)

    def load(src, slot, rows):
        return pltpu.make_async_copy(src, wbuf.at[slot, rows], wsem.at[slot])

    def whole(src, c, slot):
        load(src.at[:, cols(c)], slot, pl.ds(0, 3072)).start()

    def start_wd(m):
        for third in range(3):
            piece = 3 * m + third
            n, kq = lax.div(piece, 4), lax.rem(piece, 4)
            load(wd.at[pl.ds(pl.multiple_of(kq * 1024, 1024), 1024), cols(n)], lax.rem(6 + m, SLOTS), pl.ds(third * 1024, 1024)).start()

    def arrived(slot):
        pltpu.make_async_copy(wbuf.at[slot], wbuf.at[slot], wsem.at[slot]).wait()

    def attend(kbuf, vbuf):
        kcopy = pltpu.make_async_copy(kout, kbuf, csem.at[0])
        vcopy = pltpu.make_async_copy(vout, vbuf, csem.at[1])
        for c in range(3):
            whole(wq, c, c)
        kcopy.start()
        vcopy.start()
        norm_into(x_ref, g1_ref, u_scr)
        for c in range(3):
            arrived(c)
            q = jnp.dot(u_scr[...], wbuf[c], preferred_element_type=jnp.float32).astype(jnp.bfloat16).astype(jnp.float32)
            for j in range(4):
                part[c, :, j * 128:(j + 1) * 128] = rope(q[:, j * 128:(j + 1) * 128], cos_ref[...], sin_ref[...])
            if c < 2:
                whole((wg, wu)[c], 5, c)
            else:
                whole(wg, 6, 2)
        for j in range(3):
            for half in range(2):
                load(wo.at[:, pl.ds((2 * j + half) * 512, 512)], 3 + j, pl.ds(half * 1536, 1536)).start()

        @pl.loop(0, 5)
        def _(c):
            whole(wg, c, 6 + 2 * c)
            whole(wu, c, 7 + 2 * c)

        kcopy.wait()
        vcopy.wait()

        col = lax.broadcasted_iota(jnp.int32, (8, 512), 1)
        sub = lax.broadcasted_iota(jnp.int32, (8, 512), 0)
        own_req = (col // 64) == sub
        colpos = (col % 64) // 4 + me * 16
        diag = lax.broadcasted_iota(jnp.int32, (96, 128), 0) == lax.broadcasted_iota(jnp.int32, (96, 128), 1)
        pl.semaphore_wait(barrier, N_SP)

        def attend_group(bg):
            rows = pl.ds(pl.multiple_of(bg * 8, 8), 8)
            q = jnp.concatenate([part[h // 4, rows, (h % 4) * 128:(h % 4 + 1) * 128] for h in range(12)], axis=0).astype(jnp.bfloat16)
            k = kbuf[rows].reshape(512, 128)
            v = vbuf[rows].reshape(512, 128)
            s = lax.dot_general(q, k, (((1,), (1,)), ((), ())), preferred_element_type=jnp.float32) * (128.0 ** -0.5)
            last = jnp.zeros((8, 512), jnp.int32)
            for j in range(8):
                last = jnp.where(sub == j, seq_ref[bg * 8 + j], last)
            ok = own_req & (colpos <= last)
            weights, tops, sums = [], [], []
            for kv in range(4):
                seen = ok & ((col % 4) == kv)
                for g in range(3):
                    h = kv * 3 + g
                    masked = jnp.where(seen, s[h * 8:(h + 1) * 8, :], -1e30)
                    top = jnp.max(masked, axis=-1, keepdims=True)
                    w = jnp.where(seen, jnp.exp(masked - top), 0.0)
                    weights.append(w)
                    tops.append(jnp.broadcast_to(top, (8, 128)))
                    sums.append(jnp.broadcast_to(jnp.sum(w, axis=-1, keepdims=True), (8, 128)))
            w = jnp.concatenate(weights, axis=0).astype(jnp.bfloat16)
            mix = jnp.dot(w, v, preferred_element_type=jnp.float32)
            top_row = jnp.sum(jnp.where(diag, jnp.concatenate(tops, axis=0), 0.0), axis=0, keepdims=True)
            sum_row = jnp.sum(jnp.where(diag, jnp.concatenate(sums, axis=0), 0.0), axis=0, keepdims=True)
            for kv in range(4):
                o = kv * 12 + bg
                send[o, 0:24, :] = mix[kv * 24:(kv + 1) * 24, :]
                send[o, 24:25, :] = top_row
                send[o, 25:26, :] = sum_row

        def send_group(bg):
            for kv in range(4):
                o = kv * 12 + bg
                t = device_of(o)

                @pl.when(t != me)
                def _():
                    pltpu.make_async_remote_copy(src_ref=send.at[o], dst_ref=recv.at[me], send_sem=send_sem, recv_sem=recv_sem,
                                                 device_id={"sp": t}, device_id_type=MESH).start()

        @pl.loop(0, 12 // 2)
        def _(step):
            groups = [lax.rem(step * 2 + i + me, 12) for i in range(2)]
            for bg in groups:
                attend_group(bg)
            for bg in groups:
                send_group(bg)

    pl.run_scoped(attend, pltpu.VMEM((96, 64, 128), jnp.bfloat16), pltpu.VMEM((96, 64, 128), jnp.bfloat16))

    @pl.when(owner)
    def _():
        recv[me] = send[my_own]
        pltpu.make_async_copy(recv.at[pl.ds(0, N_SP - 1)], recv.at[pl.ds(0, N_SP - 1)], recv_sem).wait()
        top = jnp.max(recv[:, 24, :], axis=0, keepdims=True)
        f = jnp.exp(recv[:, 24, :] - top)
        tot = jnp.sum(f * recv[:, 25, :], axis=0, keepdims=True)
        fac[...] = jnp.transpose(jnp.concatenate([f, jnp.broadcast_to(tot, (64, 128))], axis=0))
        ft = fac[pl.ds(pl.multiple_of(lax.div(my_own, 12) * 24, 8), 24), :]
        acc = [jnp.zeros((24, 128), jnp.float32) for _ in range(4)]
        for i in range(N_SP):
            acc[i % 4] = acc[i % 4] + recv[i, 0:24, :] * ft[:, i:i + 1]
        total = (acc[0] + acc[1]) + (acc[2] + acc[3])
        mine[...] = (total / ft[:, 64:65]).astype(jnp.bfloat16).astype(jnp.float32)
        gath[my_own] = mine[...]

        @pl.loop(1, N_SP)
        def _(j):
            pltpu.make_async_remote_copy(src_ref=mine, dst_ref=gath.at[my_own], send_sem=gsend_sem, recv_sem=grecv_sem,
                                         device_id={"sp": lax.rem(me + j, N_SP)}, device_id_type=MESH).start()
        pltpu.make_async_copy(gath.at[pl.ds(0, N_OWN - 1)], gath.at[pl.ds(0, N_OWN - 1)], grecv_sem).wait()

    @pl.when(jnp.logical_not(owner))
    def _():
        pltpu.make_async_copy(gath, gath, grecv_sem).wait()

    def exchange(phase, n):
        return pltpu.make_async_remote_copy(src_ref=part.at[n], dst_ref=prem.at[phase, n], send_sem=psend_sem.at[n],
                                            recv_sem=precv_sem.at[phase, n], device_id={"tp": 1 - tp}, device_id_type=MESH)

    def finish(attn, hid, act):
        for kv in range(4):
            for g in range(3):
                h = kv * 3 + g
                attn[:, h * 128:(h + 1) * 128] = gath[kv * 12:(kv + 1) * 12, g * 8:(g + 1) * 8, :].reshape(96, 128).astype(jnp.bfloat16)

        for j in range(3):
            arrived(3 + j)
            for half in range(2):
                n = 2 * j + half
                part[n] = jnp.dot(attn[...], wbuf[3 + j, half * 1536:(half + 1) * 1536, :], preferred_element_type=jnp.float32)
                exchange(0, n).start()
            if j == 0:
                whole(wu, 6, 3)
            else:
                whole((wg, wu)[j - 1], 7, 3 + j)
        sq = jnp.zeros((96, 128), jnp.float32)
        for n in range(6):
            exchange(0, n).wait_recv()
            for q in range(4):
                at = slice(n * 512 + q * 128, n * 512 + (q + 1) * 128)
                here = slice(q * 128, (q + 1) * 128)
                h = (x_ref[:, at].astype(jnp.float32) + (part[n, :, here] + prem[0, n, :, here])).astype(jnp.bfloat16)
                hid[:, at] = h
                h = h.astype(jnp.float32)
                sq = sq + h * h
        inv = lax.rsqrt(jnp.sum(sq, axis=-1, keepdims=True) * (1.0 / 3072.0) + NORM_EPS)
        for c in range(24):
            at = slice(c * 128, (c + 1) * 128)
            u_scr[:, at] = (hid[:, at].astype(jnp.float32) * inv * g2_ref[c:c + 1, :].astype(jnp.float32)).astype(jnp.bfloat16)

        @pl.loop(0, 8)
        def _(c):
            sg = lax.rem(6 + 2 * c, SLOTS)
            su = lax.rem(7 + 2 * c, SLOTS)
            arrived(sg)
            gate = jnp.dot(u_scr[...], wbuf[sg], preferred_element_type=jnp.float32).astype(jnp.bfloat16).astype(jnp.float32)
            arrived(su)
            up = jnp.dot(u_scr[...], wbuf[su], preferred_element_type=jnp.float32).astype(jnp.bfloat16).astype(jnp.float32)
            act[:, cols(c)] = (gate * lax.logistic(gate) * up).astype(jnp.bfloat16)

            @pl.when(c < 4)
            def _():
                start_wd(2 * c)
                start_wd(2 * c + 1)

        waited = -1
        for n in range(6):
            total = None
            for kq in range(4):
                m, third = divmod(n * 4 + kq, 3)
                if m > waited:
                    arrived((6 + m) % SLOTS)
                    waited = m
                d = jnp.dot(act[:, kq * 1024:(kq + 1) * 1024], wbuf[(6 + m) % SLOTS, third * 1024:(third + 1) * 1024, :], preferred_element_type=jnp.float32)
                total = d if total is None else total + d
            exchange(0, n).wait_send()
            part[n] = total
            exchange(1, n).start()
        for n in range(6):
            exchange(1, n).wait_recv()
            at = slice(n * 512, (n + 1) * 512)
            y_ref[:, at] = (hid[:, at].astype(jnp.float32) + (part[n] + prem[1, n])).astype(jnp.bfloat16)

    pl.run_scoped(finish, pltpu.VMEM((96, 1536), jnp.bfloat16), pltpu.VMEM((96, 3072), jnp.bfloat16), pltpu.VMEM((96, 4096), jnp.bfloat16))

    for n in range(6):
        exchange(1, n).wait_send()

    @pl.when(owner)
    def _():
        pltpu.make_async_copy(send.at[pl.ds(0, N_OWN - 1)], send.at[pl.ds(0, N_OWN - 1)], send_sem).wait()

        @pl.loop(1, N_SP)
        def _(j):
            pltpu.make_async_copy(mine, mine, gsend_sem).wait()

    @pl.when(jnp.logical_not(owner))
    def _():
        pltpu.make_async_copy(send, send, send_sem).wait()


def main_part(seq_lens, x_tok, g_attn, g_mlp, cos2, sin2, k_out, v_out, wq, wo, wg, wu, wd):
    vmem = pl.BlockSpec(memory_space=pltpu.VMEM)
    hbm = pl.BlockSpec(memory_space=pl.ANY)
    f32, bf16 = jnp.float32, jnp.bfloat16
    return pl.pallas_call(
        main_kernel,
        out_shape=jax.ShapeDtypeStruct((96, 3072), bf16),
        in_specs=[pl.BlockSpec(memory_space=pltpu.SMEM)] + [vmem] * 5 + [hbm] * 7,
        out_specs=vmem,
        scratch_shapes=[
            pltpu.VMEM((N_OWN, MSG, 128), f32),
            pltpu.VMEM((N_SP, MSG, 128), f32),
            pltpu.VMEM((24, 128), f32),
            pltpu.VMEM((N_OWN, 24, 128), f32),
            pltpu.VMEM((128, 128), f32),
            pltpu.VMEM((6, 96, 512), f32),
            pltpu.VMEM((2, 6, 96, 512), f32),
            pltpu.VMEM((96, 3072), bf16),
            pltpu.VMEM((SLOTS, 3072, 512), bf16),
            pltpu.SemaphoreType.DMA, pltpu.SemaphoreType.DMA, pltpu.SemaphoreType.DMA, pltpu.SemaphoreType.DMA,
            pltpu.SemaphoreType.DMA((6,)), pltpu.SemaphoreType.DMA((2, 6)), pltpu.SemaphoreType.DMA((SLOTS,)), pltpu.SemaphoreType.DMA((2,)),
        ],
        compiler_params=pltpu.CompilerParams(collective_id=1, has_side_effects=True, vmem_limit_bytes=67043328),
        cost_estimate=pl.CostEstimate(flops=2 * 96 * 47_000_000, bytes_accessed=100_000_000, transcendentals=1_000_000),
        name="main_part",
    )(seq_lens, x_tok, g_attn.reshape(24, 128), g_mlp.reshape(24, 128), cos2, sin2, k_out, v_out, wq, wo, wg, wu, wd)


def solution(mesh):
    cache_spec = P(None, "sp", "tp", None)
    col_spec = P(None, "tp")
    row_spec = P("tp", None)
    full_spec = P()

    def local_step(x_tok, seq_lens, k_blk, v_blk, g_attn, wq_loc, wk_loc, wv_loc, wo_loc, g_mlp, wg_loc, wu_loc, wd_loc):
        k_out, v_out, cos2, sin2 = cache_part(seq_lens, x_tok, g_attn, k_blk, v_blk, wk_loc, wv_loc)
        y_out = main_part(seq_lens, x_tok, g_attn, g_mlp, cos2, sin2, k_out, v_out, wq_loc, wo_loc, wg_loc, wu_loc, wd_loc)
        return y_out, k_out.reshape(k_blk.shape), v_out.reshape(v_blk.shape)

    return jax.shard_map(local_step, mesh=mesh, in_specs=(full_spec, full_spec, cache_spec, cache_spec, full_spec, col_spec, col_spec, col_spec, row_spec, full_spec, col_spec, col_spec, row_spec), out_specs=(full_spec, cache_spec, cache_spec), check_vma=False)
```

```python
import jax
import jax.numpy as jnp
import numpy as np
from jax import lax
from jax.experimental import pallas as pl
from jax.experimental.pallas import tpu as pltpu
from jax.sharding import PartitionSpec as P

ROPE_BASE = 500000.0
NORM_EPS = 1e-5
N_SP = 64
N_OWN = 48
MSG = 26
SLOTS = 16
MESH = pl.DeviceIdType.MESH


def norm_into(x_ref, g_ref, out_ref):
    sq = jnp.zeros((96, 128), jnp.float32)
    for c in range(24):
        xc = x_ref[:, c * 128:(c + 1) * 128].astype(jnp.float32)
        sq = sq + xc * xc
    inv = lax.rsqrt(jnp.sum(sq, axis=-1, keepdims=True) * (1.0 / 3072.0) + NORM_EPS)
    for c in range(24):
        xc = x_ref[:, c * 128:(c + 1) * 128].astype(jnp.float32)
        out_ref[:, c * 128:(c + 1) * 128] = (xc * inv * g_ref[c:c + 1, :].astype(jnp.float32)).astype(jnp.bfloat16)


def rope(h, cos_a, sin_a):
    return (h * cos_a + pltpu.roll(h, 64, 1) * sin_a).astype(jnp.bfloat16).astype(jnp.float32)


def cache_kernel(seq_ref, x_ref, g_ref, freq_ref, kin, vin, wk, wv, kout, vout, cos_ref, sin_ref,
                 wbuf, kbuf, vbuf, u_scr, new_scr, wsem, csem, osem):
    sp = lax.axis_index("sp")
    wcopies = [pltpu.make_async_copy(w, wbuf.at[i], wsem.at[i]) for i, w in enumerate((wk, wv))]
    ccopies = [pltpu.make_async_copy(kin, kbuf, csem.at[0]), pltpu.make_async_copy(vin, vbuf, csem.at[1])]
    for copy in (wcopies[0], ccopies[0], wcopies[1], ccopies[1]):
        copy.start()
    norm_into(x_ref, g_ref, u_scr)
    u = u_scr[...]

    sub = lax.broadcasted_iota(jnp.int32, (8, 128), 0)
    low = lax.broadcasted_iota(jnp.int32, (8, 128), 1) < 64
    for bg in range(12):
        pos = jnp.zeros((8, 128), jnp.int32)
        for j in range(8):
            pos = jnp.where(sub == j, seq_ref[bg * 8 + j], pos)
        angle = pos.astype(jnp.float32) * freq_ref[...]
        cos_ref[bg * 8:(bg + 1) * 8, :] = jnp.cos(angle)
        sin_a = jnp.sin(angle)
        sin_ref[bg * 8:(bg + 1) * 8, :] = jnp.where(low, -sin_a, sin_a)

    rowpos = lax.broadcasted_iota(jnp.int32, (64, 128), 0) // 4 + sp * 16

    def update(i, buf, turn, out):
        wcopies[i].wait()
        fresh = jnp.dot(u, wbuf[i], preferred_element_type=jnp.float32).astype(jnp.bfloat16).astype(jnp.float32)
        for kv in range(4):
            rows = fresh[:, kv * 128:(kv + 1) * 128]
            rows = rope(rows, cos_ref[...], sin_ref[...]) if turn else rows
            new_scr[pl.ds(kv, 96, stride=8), :] = rows
            new_scr[pl.ds(kv + 4, 96, stride=8), :] = rows
        ccopies[i].wait()

        @pl.loop(0, 12)
        def _(bg):
            for j in range(8):
                b = bg * 8 + j
                tile = new_scr[pl.ds(pl.multiple_of(b * 8, 8), 8), :]
                wide = jnp.broadcast_to(tile[None], (8, 8, 128)).reshape(64, 128)
                buf[b] = jnp.where(rowpos == seq_ref[b], wide, buf[b].astype(jnp.float32)).astype(jnp.bfloat16)
            pltpu.make_async_copy(buf.at[pl.ds(bg * 8, 8)], out.at[pl.ds(bg * 8, 8)], osem.at[i]).start()

    update(0, kbuf, True, kout)
    update(1, vbuf, False, vout)
    pltpu.make_async_copy(kbuf, kout, osem.at[0]).wait()
    pltpu.make_async_copy(vbuf, vout, osem.at[1]).wait()


def cache_part(seq_lens, x_tok, g_attn, k_blk, v_blk, wk, wv):
    inv_freq = np.power(ROPE_BASE, np.arange(64) * (-2.0 / 128)).astype(np.float32)
    freq = jnp.asarray(np.tile(inv_freq, (8, 2)))
    vmem = pl.BlockSpec(memory_space=pltpu.VMEM)
    hbm = pl.BlockSpec(memory_space=pl.ANY)
    cache = jax.ShapeDtypeStruct((96, 64, 128), jnp.bfloat16)
    table = jax.ShapeDtypeStruct((96, 128), jnp.float32)
    return pl.pallas_call(
        cache_kernel,
        out_shape=(cache, cache, table, table),
        in_specs=[pl.BlockSpec(memory_space=pltpu.SMEM), vmem, vmem, vmem, hbm, hbm, hbm, hbm],
        out_specs=(hbm, hbm, vmem, vmem),
        scratch_shapes=[
            pltpu.VMEM((2, 3072, 512), jnp.bfloat16),
            pltpu.VMEM((96, 64, 128), jnp.bfloat16),
            pltpu.VMEM((96, 64, 128), jnp.bfloat16),
            pltpu.VMEM((96, 3072), jnp.bfloat16),
            pltpu.VMEM((768, 128), jnp.float32),
            pltpu.SemaphoreType.DMA((2,)), pltpu.SemaphoreType.DMA((2,)), pltpu.SemaphoreType.DMA((2,)),
        ],
        compiler_params=pltpu.CompilerParams(vmem_limit_bytes=67043328),
        cost_estimate=pl.CostEstimate(flops=2 * 96 * 3072 * 1024, bytes_accessed=13_000_000, transcendentals=30_000),
        name="cache_part",
    )(seq_lens, x_tok, g_attn.reshape(24, 128), freq, k_blk.reshape(96, 64, 128), v_blk.reshape(96, 64, 128), wk, wv)


def main_kernel(seq_ref, x_ref, g1_ref, g2_ref, cos_ref, sin_ref, kout, vout, wq, wo, wg, wu, wd, y_ref,
                send, recv, mine, gath, fac, part, prem, u_scr, wbuf,
                send_sem, recv_sem, gsend_sem, grecv_sem, psend_sem, precv_sem, wsem, csem, ysem):
    me = lax.axis_index("sp")
    tp = lax.axis_index("tp")
    barrier = pltpu.get_barrier_semaphore()

    def turn_of(t):
        return lax.rem(lax.rem(t, 4) + lax.rem(lax.div(t, 4), 4) + lax.div(t, 16), 4)

    owner = turn_of(me) < 3
    my_own = lax.div(me, 4) * 3 + turn_of(me)

    def device_of(o):
        yz = lax.div(o, 3)
        return yz * 4 + lax.rem(lax.rem(o, 3) + 8 - lax.rem(yz, 4) - lax.div(yz, 4), 4)

    @pl.loop(1, N_SP)
    def _(j):
        pl.semaphore_signal(barrier, inc=1, device_id={"sp": lax.rem(me + j, N_SP)}, device_id_type=MESH)
    pl.semaphore_signal(barrier, inc=1, device_id={"tp": 1 - tp}, device_id_type=MESH)

    def cols(c):
        return pl.ds(pl.multiple_of(c * 512, 512), 512)

    def load(src, slot, rows):
        return pltpu.make_async_copy(src, wbuf.at[slot, rows], wsem.at[slot])

    def whole(src, c, slot):
        load(src.at[:, cols(c)], slot, pl.ds(0, 3072)).start()

    def start_wd(m):
        for third in range(3):
            piece = 3 * m + third
            n, kq = lax.div(piece, 4), lax.rem(piece, 4)
            load(wd.at[pl.ds(pl.multiple_of(kq * 1024, 1024), 1024), cols(n)], 5 + m, pl.ds(third * 1024, 1024)).start()

    def arrived(slot):
        pltpu.make_async_copy(wbuf.at[slot], wbuf.at[slot], wsem.at[slot]).wait()

    def attend(kbuf, vbuf):
        kcopy = pltpu.make_async_copy(kout, kbuf, csem.at[0])
        vcopy = pltpu.make_async_copy(vout, vbuf, csem.at[1])
        for c in range(3):
            whole(wq, c, c)
        kcopy.start()
        vcopy.start()
        norm_into(x_ref, g1_ref, u_scr)
        for c in range(3):
            arrived(c)
            q = jnp.dot(u_scr[...], wbuf[c], preferred_element_type=jnp.float32).astype(jnp.bfloat16).astype(jnp.float32)
            for j in range(4):
                part[c, :, j * 128:(j + 1) * 128] = rope(q[:, j * 128:(j + 1) * 128], cos_ref[...], sin_ref[...])
            if c < 2:
                whole((wg, wu)[c], 5, c)
            else:
                whole(wg, 6, 2)
        for j in range(3):
            for half in range(2):
                load(wo.at[:, pl.ds((2 * j + half) * 512, 512)], 3 + j, pl.ds(half * 1536, 1536)).start()

        @pl.loop(0, 5)
        def _(c):
            whole(wg, c, 6 + 2 * c)
            whole(wu, c, 7 + 2 * c)

        kcopy.wait()
        vcopy.wait()

        col = lax.broadcasted_iota(jnp.int32, (8, 512), 1)
        sub = lax.broadcasted_iota(jnp.int32, (8, 512), 0)
        own_req = (col // 64) == sub
        colpos = (col % 64) // 4 + me * 16
        diag = lax.broadcasted_iota(jnp.int32, (96, 128), 0) == lax.broadcasted_iota(jnp.int32, (96, 128), 1)
        pl.semaphore_wait(barrier, N_SP)

        def attend_group(bg):
            rows = pl.ds(pl.multiple_of(bg * 8, 8), 8)
            q = jnp.concatenate([part[h // 4, rows, (h % 4) * 128:(h % 4 + 1) * 128] for h in range(12)], axis=0).astype(jnp.bfloat16)
            k = kbuf[rows].reshape(512, 128)
            v = vbuf[rows].reshape(512, 128)
            s = lax.dot_general(q, k, (((1,), (1,)), ((), ())), preferred_element_type=jnp.float32) * (128.0 ** -0.5)
            last = jnp.zeros((8, 512), jnp.int32)
            for j in range(8):
                last = jnp.where(sub == j, seq_ref[bg * 8 + j], last)
            ok = own_req & (colpos <= last)
            weights, tops, sums = [], [], []
            for kv in range(4):
                seen = ok & ((col % 4) == kv)
                for g in range(3):
                    h = kv * 3 + g
                    masked = jnp.where(seen, s[h * 8:(h + 1) * 8, :], -1e30)
                    top = jnp.max(masked, axis=-1, keepdims=True)
                    w = jnp.where(seen, jnp.exp(masked - top), 0.0)
                    weights.append(w)
                    tops.append(jnp.broadcast_to(top, (8, 128)))
                    sums.append(jnp.broadcast_to(jnp.sum(w, axis=-1, keepdims=True), (8, 128)))
            w = jnp.concatenate(weights, axis=0).astype(jnp.bfloat16)
            mix = jnp.dot(w, v, preferred_element_type=jnp.float32)
            top_row = jnp.sum(jnp.where(diag, jnp.concatenate(tops, axis=0), 0.0), axis=0, keepdims=True)
            sum_row = jnp.sum(jnp.where(diag, jnp.concatenate(sums, axis=0), 0.0), axis=0, keepdims=True)
            for kv in range(4):
                o = kv * 12 + bg
                send[o, 0:24, :] = mix[kv * 24:(kv + 1) * 24, :]
                send[o, 24:25, :] = top_row
                send[o, 25:26, :] = sum_row

        def send_group(bg):
            for kv in range(4):
                o = kv * 12 + bg
                t = device_of(o)

                @pl.when(t != me)
                def _():
                    pltpu.make_async_remote_copy(src_ref=send.at[o], dst_ref=recv.at[me], send_sem=send_sem, recv_sem=recv_sem,
                                                 device_id={"sp": t}, device_id_type=MESH).start()

        @pl.loop(0, 12 // 2)
        def _(step):
            groups = [lax.rem(step * 2 + i + me, 12) for i in range(2)]
            for bg in groups:
                attend_group(bg)
            for bg in groups:
                send_group(bg)

    pl.run_scoped(attend, pltpu.VMEM((96, 64, 128), jnp.bfloat16), pltpu.VMEM((96, 64, 128), jnp.bfloat16))

    def exchange(phase, n):
        return pltpu.make_async_remote_copy(src_ref=part.at[n], dst_ref=prem.at[phase, n], send_sem=psend_sem.at[n],
                                            recv_sem=precv_sem.at[phase, n], device_id={"tp": 1 - tp}, device_id_type=MESH)

    def finish(attn, hid, act, extra):
        pltpu.make_async_copy(wu.at[:, pl.ds(6 * 512, 512)], extra, wsem.at[SLOTS]).start()

        @pl.when(owner)
        def _():
            recv[me] = send[my_own]
            pltpu.make_async_copy(recv.at[pl.ds(0, N_SP - 1)], recv.at[pl.ds(0, N_SP - 1)], recv_sem).wait()
            top = jnp.max(recv[:, 24, :], axis=0, keepdims=True)
            f = jnp.exp(recv[:, 24, :] - top)
            tot = jnp.sum(f * recv[:, 25, :], axis=0, keepdims=True)
            fac[...] = jnp.transpose(jnp.concatenate([f, jnp.broadcast_to(tot, (64, 128))], axis=0))
            ft = fac[pl.ds(pl.multiple_of(lax.div(my_own, 12) * 24, 8), 24), :]
            acc = [jnp.zeros((24, 128), jnp.float32) for _ in range(4)]
            for i in range(N_SP):
                acc[i % 4] = acc[i % 4] + recv[i, 0:24, :] * ft[:, i:i + 1]
            total = (acc[0] + acc[1]) + (acc[2] + acc[3])
            mine[...] = (total / ft[:, 64:65]).astype(jnp.bfloat16).astype(jnp.float32)
            gath[my_own] = mine[...]

            @pl.loop(1, N_SP)
            def _(j):
                pltpu.make_async_remote_copy(src_ref=mine, dst_ref=gath.at[my_own], send_sem=gsend_sem, recv_sem=grecv_sem,
                                             device_id={"sp": lax.rem(me + j, N_SP)}, device_id_type=MESH).start()
            pltpu.make_async_copy(gath.at[pl.ds(0, N_OWN - 1)], gath.at[pl.ds(0, N_OWN - 1)], grecv_sem).wait()

        @pl.when(jnp.logical_not(owner))
        def _():
            pltpu.make_async_copy(gath, gath, grecv_sem).wait()

        for kv in range(4):
            for g in range(3):
                h = kv * 3 + g
                attn[:, h * 128:(h + 1) * 128] = gath[kv * 12:(kv + 1) * 12, g * 8:(g + 1) * 8, :].reshape(96, 128).astype(jnp.bfloat16)

        for j in range(3):
            arrived(3 + j)
            for half in range(2):
                n = 2 * j + half
                part[n] = jnp.dot(attn[...], wbuf[3 + j, half * 1536:(half + 1) * 1536, :], preferred_element_type=jnp.float32)
                exchange(0, n).start()
            if j < 2:
                whole((wg, wu)[j], 7, 3 + j)
            else:
                start_wd(0)
        sq = jnp.zeros((96, 128), jnp.float32)
        for n in range(6):
            exchange(0, n).wait_recv()
            for q in range(4):
                at = slice(n * 512 + q * 128, n * 512 + (q + 1) * 128)
                here = slice(q * 128, (q + 1) * 128)
                h = (x_ref[:, at].astype(jnp.float32) + (part[n, :, here] + prem[0, n, :, here])).astype(jnp.bfloat16)
                hid[:, at] = h
                h = h.astype(jnp.float32)
                sq = sq + h * h
        inv = lax.rsqrt(jnp.sum(sq, axis=-1, keepdims=True) * (1.0 / 3072.0) + NORM_EPS)
        for c in range(24):
            at = slice(c * 128, (c + 1) * 128)
            u_scr[:, at] = (hid[:, at].astype(jnp.float32) * inv * g2_ref[c:c + 1, :].astype(jnp.float32)).astype(jnp.bfloat16)

        def gate_up(c, gate_ref, gate_sem, up_ref, up_sem):
            pltpu.make_async_copy(gate_ref, gate_ref, wsem.at[gate_sem]).wait()
            gate = jnp.dot(u_scr[...], gate_ref[...], preferred_element_type=jnp.float32).astype(jnp.bfloat16).astype(jnp.float32)
            pltpu.make_async_copy(up_ref, up_ref, wsem.at[up_sem]).wait()
            up = jnp.dot(u_scr[...], up_ref[...], preferred_element_type=jnp.float32).astype(jnp.bfloat16).astype(jnp.float32)
            act[:, cols(c)] = (gate * lax.logistic(gate) * up).astype(jnp.bfloat16)

        @pl.loop(0, 5)
        def _(c):
            gate_up(c, wbuf.at[6 + 2 * c], 6 + 2 * c, wbuf.at[7 + 2 * c], 7 + 2 * c)

            @pl.when(c < 4)
            def _():
                start_wd(2 * c + 1)

            @pl.when(c < 3)
            def _():
                start_wd(2 * c + 2)

        gate_up(5, wbuf.at[0], 0, wbuf.at[1], 1)
        gate_up(6, wbuf.at[2], 2, extra, SLOTS)
        gate_up(7, wbuf.at[3], 3, wbuf.at[4], 4)

        waited = -1
        for n in range(6):
            total = None
            for kq in range(4):
                m, third = divmod(n * 4 + kq, 3)
                if m > waited:
                    arrived(5 + m)
                    waited = m
                d = jnp.dot(act[:, kq * 1024:(kq + 1) * 1024], wbuf[5 + m, third * 1024:(third + 1) * 1024, :], preferred_element_type=jnp.float32)
                total = d if total is None else total + d
            exchange(0, n).wait_send()
            part[n] = total
            exchange(1, n).start()
        for n in range(6):
            exchange(1, n).wait_recv()
            at = pl.ds(n * 512, 512)
            hid[:, at] = (hid[:, at].astype(jnp.float32) + (part[n] + prem[1, n])).astype(jnp.bfloat16)
            pltpu.make_async_copy(hid.at[:, at], y_ref.at[:, at], ysem).start()
        pltpu.make_async_copy(hid, y_ref, ysem).wait()

    pl.run_scoped(finish, pltpu.VMEM((96, 1536), jnp.bfloat16), pltpu.VMEM((96, 3072), jnp.bfloat16), pltpu.VMEM((96, 4096), jnp.bfloat16),
                  pltpu.VMEM((3072, 512), jnp.bfloat16))

    for n in range(6):
        exchange(1, n).wait_send()

    @pl.when(owner)
    def _():
        pltpu.make_async_copy(send.at[pl.ds(0, N_OWN - 1)], send.at[pl.ds(0, N_OWN - 1)], send_sem).wait()

        @pl.loop(1, N_SP)
        def _(j):
            pltpu.make_async_copy(mine, mine, gsend_sem).wait()

    @pl.when(jnp.logical_not(owner))
    def _():
        pltpu.make_async_copy(send, send, send_sem).wait()


def main_part(seq_lens, x_tok, g_attn, g_mlp, cos2, sin2, k_out, v_out, wq, wo, wg, wu, wd):
    vmem = pl.BlockSpec(memory_space=pltpu.VMEM)
    hbm = pl.BlockSpec(memory_space=pl.ANY)
    f32, bf16 = jnp.float32, jnp.bfloat16
    return pl.pallas_call(
        main_kernel,
        out_shape=jax.ShapeDtypeStruct((96, 3072), bf16),
        in_specs=[pl.BlockSpec(memory_space=pltpu.SMEM)] + [vmem] * 5 + [hbm] * 7,
        out_specs=hbm,
        scratch_shapes=[
            pltpu.VMEM((N_OWN, MSG, 128), f32),
            pltpu.VMEM((N_SP, MSG, 128), f32),
            pltpu.VMEM((24, 128), f32),
            pltpu.VMEM((N_OWN, 24, 128), f32),
            pltpu.VMEM((128, 128), f32),
            pltpu.VMEM((6, 96, 512), f32),
            pltpu.VMEM((2, 6, 96, 512), f32),
            pltpu.VMEM((96, 3072), bf16),
            pltpu.VMEM((SLOTS, 3072, 512), bf16),
            pltpu.SemaphoreType.DMA, pltpu.SemaphoreType.DMA, pltpu.SemaphoreType.DMA, pltpu.SemaphoreType.DMA,
            pltpu.SemaphoreType.DMA((6,)), pltpu.SemaphoreType.DMA((2, 6)), pltpu.SemaphoreType.DMA((SLOTS + 1,)), pltpu.SemaphoreType.DMA((2,)), pltpu.SemaphoreType.DMA,
        ],
        compiler_params=pltpu.CompilerParams(collective_id=1, has_side_effects=True, vmem_limit_bytes=67043328),
        cost_estimate=pl.CostEstimate(flops=2 * 96 * 47_000_000, bytes_accessed=100_000_000, transcendentals=1_000_000),
        name="main_part",
    )(seq_lens, x_tok, g_attn.reshape(24, 128), g_mlp.reshape(24, 128), cos2, sin2, k_out, v_out, wq, wo, wg, wu, wd)


def solution(mesh):
    cache_spec = P(None, "sp", "tp", None)
    col_spec = P(None, "tp")
    row_spec = P("tp", None)
    full_spec = P()

    def local_step(x_tok, seq_lens, k_blk, v_blk, g_attn, wq_loc, wk_loc, wv_loc, wo_loc, g_mlp, wg_loc, wu_loc, wd_loc):
        k_out, v_out, cos2, sin2 = cache_part(seq_lens, x_tok, g_attn, k_blk, v_blk, wk_loc, wv_loc)
        y_out = main_part(seq_lens, x_tok, g_attn, g_mlp, cos2, sin2, k_out, v_out, wq_loc, wo_loc, wg_loc, wu_loc, wd_loc)
        return y_out, k_out.reshape(k_blk.shape), v_out.reshape(v_blk.shape)

    return jax.shard_map(local_step, mesh=mesh, in_specs=(full_spec, full_spec, cache_spec, cache_spec, full_spec, col_spec, col_spec, col_spec, row_spec, full_spec, col_spec, col_spec, row_spec), out_specs=(full_spec, cache_spec, cache_spec), check_vma=False)
```

```python
import jax
import jax.numpy as jnp
import numpy as np
from jax import lax
from jax.experimental import pallas as pl
from jax.experimental.pallas import tpu as pltpu
from jax.sharding import PartitionSpec as P

ROPE_BASE = 500000.0
NORM_EPS = 1e-5
N_SP = 64
N_OWN = 48
MSG = 26
SLOTS = 16
MESH = pl.DeviceIdType.MESH


def norm_into(x_ref, g_ref, out_ref):
    sq = jnp.zeros((96, 128), jnp.float32)
    for c in range(24):
        xc = x_ref[:, c * 128:(c + 1) * 128].astype(jnp.float32)
        sq = sq + xc * xc
    inv = lax.rsqrt(jnp.sum(sq, axis=-1, keepdims=True) * (1.0 / 3072.0) + NORM_EPS)
    for c in range(24):
        xc = x_ref[:, c * 128:(c + 1) * 128].astype(jnp.float32)
        out_ref[:, c * 128:(c + 1) * 128] = (xc * inv * g_ref[c:c + 1, :].astype(jnp.float32)).astype(jnp.bfloat16)


def rope(h, cos_a, sin_a):
    return (h * cos_a + pltpu.roll(h, 64, 1) * sin_a).astype(jnp.bfloat16).astype(jnp.float32)


def cache_kernel(seq_ref, x_ref, g_ref, freq_ref, kin, vin, wk, wv, kout, vout, cos_ref, sin_ref,
                 wbuf, kbuf, vbuf, u_scr, new_scr, wsem, csem, osem):
    sp = lax.axis_index("sp")
    wcopies = [pltpu.make_async_copy(w, wbuf.at[i], wsem.at[i]) for i, w in enumerate((wk, wv))]
    ccopies = [pltpu.make_async_copy(kin, kbuf, csem.at[0]), pltpu.make_async_copy(vin, vbuf, csem.at[1])]
    for copy in (wcopies[0], ccopies[0], wcopies[1], ccopies[1]):
        copy.start()
    norm_into(x_ref, g_ref, u_scr)
    u = u_scr[...]

    sub = lax.broadcasted_iota(jnp.int32, (8, 128), 0)
    low = lax.broadcasted_iota(jnp.int32, (8, 128), 1) < 64
    for bg in range(12):
        pos = jnp.zeros((8, 128), jnp.int32)
        for j in range(8):
            pos = jnp.where(sub == j, seq_ref[bg * 8 + j], pos)
        angle = pos.astype(jnp.float32) * freq_ref[...]
        cos_ref[bg * 8:(bg + 1) * 8, :] = jnp.cos(angle)
        sin_a = jnp.sin(angle)
        sin_ref[bg * 8:(bg + 1) * 8, :] = jnp.where(low, -sin_a, sin_a)

    rowpos = lax.broadcasted_iota(jnp.int32, (64, 128), 0) // 4 + sp * 16

    def update(i, buf, turn, out):
        wcopies[i].wait()
        fresh = jnp.dot(u, wbuf[i], preferred_element_type=jnp.float32).astype(jnp.bfloat16).astype(jnp.float32)
        for kv in range(4):
            rows = fresh[:, kv * 128:(kv + 1) * 128]
            rows = rope(rows, cos_ref[...], sin_ref[...]) if turn else rows
            new_scr[pl.ds(kv, 96, stride=8), :] = rows
            new_scr[pl.ds(kv + 4, 96, stride=8), :] = rows
        ccopies[i].wait()

        @pl.loop(0, 12)
        def _(bg):
            for j in range(8):
                b = bg * 8 + j
                tile = new_scr[pl.ds(pl.multiple_of(b * 8, 8), 8), :]
                wide = jnp.broadcast_to(tile[None], (8, 8, 128)).reshape(64, 128)
                buf[b] = jnp.where(rowpos == seq_ref[b], wide, buf[b].astype(jnp.float32)).astype(jnp.bfloat16)
            pltpu.make_async_copy(buf.at[pl.ds(bg * 8, 8)], out.at[pl.ds(bg * 8, 8)], osem.at[i]).start()

    update(0, kbuf, True, kout)
    update(1, vbuf, False, vout)
    pltpu.make_async_copy(kbuf, kout, osem.at[0]).wait()
    pltpu.make_async_copy(vbuf, vout, osem.at[1]).wait()


def cache_part(seq_lens, x_tok, g_attn, k_blk, v_blk, wk, wv):
    inv_freq = np.power(ROPE_BASE, np.arange(64) * (-2.0 / 128)).astype(np.float32)
    freq = jnp.asarray(np.tile(inv_freq, (8, 2)))
    vmem = pl.BlockSpec(memory_space=pltpu.VMEM)
    hbm = pl.BlockSpec(memory_space=pl.ANY)
    cache = jax.ShapeDtypeStruct((96, 64, 128), jnp.bfloat16)
    table = jax.ShapeDtypeStruct((96, 128), jnp.float32)
    return pl.pallas_call(
        cache_kernel,
        out_shape=(cache, cache, table, table),
        in_specs=[pl.BlockSpec(memory_space=pltpu.SMEM), vmem, vmem, vmem, hbm, hbm, hbm, hbm],
        out_specs=(hbm, hbm, vmem, vmem),
        scratch_shapes=[
            pltpu.VMEM((2, 3072, 512), jnp.bfloat16),
            pltpu.VMEM((96, 64, 128), jnp.bfloat16),
            pltpu.VMEM((96, 64, 128), jnp.bfloat16),
            pltpu.VMEM((96, 3072), jnp.bfloat16),
            pltpu.VMEM((768, 128), jnp.float32),
            pltpu.SemaphoreType.DMA((2,)), pltpu.SemaphoreType.DMA((2,)), pltpu.SemaphoreType.DMA((2,)),
        ],
        compiler_params=pltpu.CompilerParams(vmem_limit_bytes=67043328),
        cost_estimate=pl.CostEstimate(flops=2 * 96 * 3072 * 1024, bytes_accessed=13_000_000, transcendentals=30_000),
        name="cache_part",
    )(seq_lens, x_tok, g_attn.reshape(24, 128), freq, k_blk.reshape(96, 64, 128), v_blk.reshape(96, 64, 128), wk, wv)


def main_kernel(seq_ref, x_ref, g1_ref, g2_ref, cos_ref, sin_ref, kout, vout, wq, wo, wg, wu, wd, y_ref,
                send, recv, mine, gath, fac, part, prem, u_scr, wbuf,
                send_sem, recv_sem, gsend_sem, grecv_sem, psend_sem, precv_sem, wsem, csem, ysem):
    me = lax.axis_index("sp")
    tp = lax.axis_index("tp")
    barrier = pltpu.get_barrier_semaphore()

    def turn_of(t):
        return lax.rem(lax.rem(t, 4) + lax.rem(lax.div(t, 4), 4) + lax.div(t, 16), 4)

    owner = turn_of(me) < 3
    my_own = lax.div(me, 4) * 3 + turn_of(me)

    def device_of(o):
        yz = lax.div(o, 3)
        return yz * 4 + lax.rem(lax.rem(o, 3) + 8 - lax.rem(yz, 4) - lax.div(yz, 4), 4)

    @pl.loop(1, N_SP)
    def _(j):
        pl.semaphore_signal(barrier, inc=1, device_id={"sp": lax.rem(me + j, N_SP)}, device_id_type=MESH)
    pl.semaphore_signal(barrier, inc=1, device_id={"tp": 1 - tp}, device_id_type=MESH)

    def cols(c):
        return pl.ds(pl.multiple_of(c * 512, 512), 512)

    def load(src, slot, rows):
        return pltpu.make_async_copy(src, wbuf.at[slot, rows], wsem.at[slot])

    def whole(src, c, slot):
        load(src.at[:, cols(c)], slot, pl.ds(0, 3072)).start()

    def start_wd(m):
        for third in range(3):
            piece = 3 * m + third
            n, kq = lax.div(piece, 4), lax.rem(piece, 4)
            load(wd.at[pl.ds(pl.multiple_of(kq * 1024, 1024), 1024), cols(n)], 5 + m, pl.ds(third * 1024, 1024)).start()

    def arrived(slot):
        pltpu.make_async_copy(wbuf.at[slot], wbuf.at[slot], wsem.at[slot]).wait()

    def attend(kbuf, vbuf):
        kcopy = pltpu.make_async_copy(kout, kbuf, csem.at[0])
        vcopy = pltpu.make_async_copy(vout, vbuf, csem.at[1])
        for c in range(3):
            whole(wq, c, c)
        kcopy.start()
        vcopy.start()
        norm_into(x_ref, g1_ref, u_scr)
        for c in range(3):
            arrived(c)
            q = jnp.dot(u_scr[...], wbuf[c], preferred_element_type=jnp.float32).astype(jnp.bfloat16).astype(jnp.float32)
            for j in range(4):
                part[c, :, j * 128:(j + 1) * 128] = rope(q[:, j * 128:(j + 1) * 128], cos_ref[...], sin_ref[...])
            if c < 2:
                whole((wg, wu)[c], 5, c)
            else:
                whole(wg, 6, 2)
        for j in range(3):
            for half in range(2):
                load(wo.at[:, pl.ds((2 * j + half) * 512, 512)], 3 + j, pl.ds(half * 1536, 1536)).start()

        @pl.loop(0, 5)
        def _(c):
            whole(wg, c, 6 + 2 * c)
            whole(wu, c, 7 + 2 * c)

        kcopy.wait()
        vcopy.wait()

        col = lax.broadcasted_iota(jnp.int32, (8, 512), 1)
        sub = lax.broadcasted_iota(jnp.int32, (8, 512), 0)
        own_req = (col // 64) == sub
        colpos = (col % 64) // 4 + me * 16
        diag = lax.broadcasted_iota(jnp.int32, (96, 128), 0) == lax.broadcasted_iota(jnp.int32, (96, 128), 1)
        pl.semaphore_wait(barrier, N_SP)

        def attend_group(bg):
            rows = pl.ds(pl.multiple_of(bg * 8, 8), 8)
            q = jnp.concatenate([part[h // 4, rows, (h % 4) * 128:(h % 4 + 1) * 128] for h in range(12)], axis=0).astype(jnp.bfloat16)
            k = kbuf[rows].reshape(512, 128)
            v = vbuf[rows].reshape(512, 128)
            s = lax.dot_general(q, k, (((1,), (1,)), ((), ())), preferred_element_type=jnp.float32) * (128.0 ** -0.5)
            last = jnp.zeros((8, 512), jnp.int32)
            for j in range(8):
                last = jnp.where(sub == j, seq_ref[bg * 8 + j], last)
            ok = own_req & (colpos <= last)
            weights, tops, sums = [], [], []
            for kv in range(4):
                seen = ok & ((col % 4) == kv)
                for g in range(3):
                    h = kv * 3 + g
                    masked = jnp.where(seen, s[h * 8:(h + 1) * 8, :], -1e30)
                    top = jnp.max(masked, axis=-1, keepdims=True)
                    w = jnp.where(seen, jnp.exp(masked - top), 0.0)
                    weights.append(w)
                    tops.append(jnp.broadcast_to(top, (8, 128)))
                    sums.append(jnp.broadcast_to(jnp.sum(w, axis=-1, keepdims=True), (8, 128)))
            w = jnp.concatenate(weights, axis=0).astype(jnp.bfloat16)
            mix = jnp.dot(w, v, preferred_element_type=jnp.float32)
            top_row = jnp.sum(jnp.where(diag, jnp.concatenate(tops, axis=0), 0.0), axis=0, keepdims=True)
            sum_row = jnp.sum(jnp.where(diag, jnp.concatenate(sums, axis=0), 0.0), axis=0, keepdims=True)
            for kv in range(4):
                o = kv * 12 + bg
                send[o, 0:24, :] = mix[kv * 24:(kv + 1) * 24, :]
                send[o, 24:25, :] = top_row
                send[o, 25:26, :] = sum_row

        def send_group(bg):
            for kv in range(4):
                o = kv * 12 + bg
                t = device_of(o)

                @pl.when(t != me)
                def _():
                    pltpu.make_async_remote_copy(src_ref=send.at[o], dst_ref=recv.at[me], send_sem=send_sem, recv_sem=recv_sem,
                                                 device_id={"sp": t}, device_id_type=MESH).start()

        @pl.loop(0, 12 // 3)
        def _(step):
            groups = [lax.rem(step * 3 + i + me, 12) for i in range(3)]
            for bg in groups:
                attend_group(bg)
            for bg in groups:
                send_group(bg)

    pl.run_scoped(attend, pltpu.VMEM((96, 64, 128), jnp.bfloat16), pltpu.VMEM((96, 64, 128), jnp.bfloat16))

    def exchange(phase, n):
        return pltpu.make_async_remote_copy(src_ref=part.at[n], dst_ref=prem.at[phase, n], send_sem=psend_sem.at[n],
                                            recv_sem=precv_sem.at[phase, n], device_id={"tp": 1 - tp}, device_id_type=MESH)

    def finish(attn, hid, act, extra):
        pltpu.make_async_copy(wu.at[:, pl.ds(6 * 512, 512)], extra, wsem.at[SLOTS]).start()

        @pl.when(owner)
        def _():
            recv[me] = send[my_own]
            pltpu.make_async_copy(recv.at[pl.ds(0, N_SP - 1)], recv.at[pl.ds(0, N_SP - 1)], recv_sem).wait()
            top = jnp.max(recv[:, 24, :], axis=0, keepdims=True)
            f = jnp.exp(recv[:, 24, :] - top)
            tot = jnp.sum(f * recv[:, 25, :], axis=0, keepdims=True)
            fac[...] = jnp.transpose(jnp.concatenate([f, jnp.broadcast_to(tot, (64, 128))], axis=0))
            ft = fac[pl.ds(pl.multiple_of(lax.div(my_own, 12) * 24, 8), 24), :]
            acc = [jnp.zeros((24, 128), jnp.float32) for _ in range(4)]
            for i in range(N_SP):
                acc[i % 4] = acc[i % 4] + recv[i, 0:24, :] * ft[:, i:i + 1]
            total = (acc[0] + acc[1]) + (acc[2] + acc[3])
            mine[...] = (total / ft[:, 64:65]).astype(jnp.bfloat16).astype(jnp.float32)
            gath[my_own] = mine[...]

            @pl.loop(1, N_SP)
            def _(j):
                pltpu.make_async_remote_copy(src_ref=mine, dst_ref=gath.at[my_own], send_sem=gsend_sem, recv_sem=grecv_sem,
                                             device_id={"sp": lax.rem(me + j, N_SP)}, device_id_type=MESH).start()
            pltpu.make_async_copy(gath.at[pl.ds(0, N_OWN - 1)], gath.at[pl.ds(0, N_OWN - 1)], grecv_sem).wait()

        @pl.when(jnp.logical_not(owner))
        def _():
            pltpu.make_async_copy(gath, gath, grecv_sem).wait()

        for kv in range(4):
            for g in range(3):
                h = kv * 3 + g
                attn[:, h * 128:(h + 1) * 128] = gath[kv * 12:(kv + 1) * 12, g * 8:(g + 1) * 8, :].reshape(96, 128).astype(jnp.bfloat16)

        for j in range(3):
            arrived(3 + j)
            for half in range(2):
                n = 2 * j + half
                part[n] = jnp.dot(attn[...], wbuf[3 + j, half * 1536:(half + 1) * 1536, :], preferred_element_type=jnp.float32)
                exchange(0, n).start()
            if j < 2:
                whole((wg, wu)[j], 7, 3 + j)
            else:
                start_wd(0)
        sq = jnp.zeros((96, 128), jnp.float32)
        for n in range(6):
            exchange(0, n).wait_recv()
            for q in range(4):
                at = slice(n * 512 + q * 128, n * 512 + (q + 1) * 128)
                here = slice(q * 128, (q + 1) * 128)
                h = (x_ref[:, at].astype(jnp.float32) + (part[n, :, here] + prem[0, n, :, here])).astype(jnp.bfloat16)
                hid[:, at] = h
                h = h.astype(jnp.float32)
                sq = sq + h * h
        inv = lax.rsqrt(jnp.sum(sq, axis=-1, keepdims=True) * (1.0 / 3072.0) + NORM_EPS)
        for c in range(24):
            at = slice(c * 128, (c + 1) * 128)
            u_scr[:, at] = (hid[:, at].astype(jnp.float32) * inv * g2_ref[c:c + 1, :].astype(jnp.float32)).astype(jnp.bfloat16)

        def gate_up(c, gate_ref, gate_sem, up_ref, up_sem):
            pltpu.make_async_copy(gate_ref, gate_ref, wsem.at[gate_sem]).wait()
            gate = jnp.dot(u_scr[...], gate_ref[...], preferred_element_type=jnp.float32).astype(jnp.bfloat16).astype(jnp.float32)
            pltpu.make_async_copy(up_ref, up_ref, wsem.at[up_sem]).wait()
            up = jnp.dot(u_scr[...], up_ref[...], preferred_element_type=jnp.float32).astype(jnp.bfloat16).astype(jnp.float32)
            act[:, cols(c)] = (gate * lax.logistic(gate) * up).astype(jnp.bfloat16)

        @pl.loop(0, 5)
        def _(c):
            gate_up(c, wbuf.at[6 + 2 * c], 6 + 2 * c, wbuf.at[7 + 2 * c], 7 + 2 * c)

            @pl.when(c < 4)
            def _():
                start_wd(2 * c + 1)

            @pl.when(c < 3)
            def _():
                start_wd(2 * c + 2)

        gate_up(5, wbuf.at[0], 0, wbuf.at[1], 1)
        gate_up(6, wbuf.at[2], 2, extra, SLOTS)
        gate_up(7, wbuf.at[3], 3, wbuf.at[4], 4)

        waited = -1
        for n in range(6):
            total = None
            for kq in range(4):
                m, third = divmod(n * 4 + kq, 3)
                if m > waited:
                    arrived(5 + m)
                    waited = m
                d = jnp.dot(act[:, kq * 1024:(kq + 1) * 1024], wbuf[5 + m, third * 1024:(third + 1) * 1024, :], preferred_element_type=jnp.float32)
                total = d if total is None else total + d
            exchange(0, n).wait_send()
            part[n] = total
            exchange(1, n).start()
        for n in range(6):
            exchange(1, n).wait_recv()
            at = pl.ds(n * 512, 512)
            hid[:, at] = (hid[:, at].astype(jnp.float32) + (part[n] + prem[1, n])).astype(jnp.bfloat16)
            pltpu.make_async_copy(hid.at[:, at], y_ref.at[:, at], ysem).start()
        pltpu.make_async_copy(hid, y_ref, ysem).wait()

    pl.run_scoped(finish, pltpu.VMEM((96, 1536), jnp.bfloat16), pltpu.VMEM((96, 3072), jnp.bfloat16), pltpu.VMEM((96, 4096), jnp.bfloat16),
                  pltpu.VMEM((3072, 512), jnp.bfloat16))

    for n in range(6):
        exchange(1, n).wait_send()

    @pl.when(owner)
    def _():
        pltpu.make_async_copy(send.at[pl.ds(0, N_OWN - 1)], send.at[pl.ds(0, N_OWN - 1)], send_sem).wait()

        @pl.loop(1, N_SP)
        def _(j):
            pltpu.make_async_copy(mine, mine, gsend_sem).wait()

    @pl.when(jnp.logical_not(owner))
    def _():
        pltpu.make_async_copy(send, send, send_sem).wait()


def main_part(seq_lens, x_tok, g_attn, g_mlp, cos2, sin2, k_out, v_out, wq, wo, wg, wu, wd):
    vmem = pl.BlockSpec(memory_space=pltpu.VMEM)
    hbm = pl.BlockSpec(memory_space=pl.ANY)
    f32, bf16 = jnp.float32, jnp.bfloat16
    return pl.pallas_call(
        main_kernel,
        out_shape=jax.ShapeDtypeStruct((96, 3072), bf16),
        in_specs=[pl.BlockSpec(memory_space=pltpu.SMEM)] + [vmem] * 5 + [hbm] * 7,
        out_specs=hbm,
        scratch_shapes=[
            pltpu.VMEM((N_OWN, MSG, 128), f32),
            pltpu.VMEM((N_SP, MSG, 128), f32),
            pltpu.VMEM((24, 128), f32),
            pltpu.VMEM((N_OWN, 24, 128), f32),
            pltpu.VMEM((128, 128), f32),
            pltpu.VMEM((6, 96, 512), f32),
            pltpu.VMEM((2, 6, 96, 512), f32),
            pltpu.VMEM((96, 3072), bf16),
            pltpu.VMEM((SLOTS, 3072, 512), bf16),
            pltpu.SemaphoreType.DMA, pltpu.SemaphoreType.DMA, pltpu.SemaphoreType.DMA, pltpu.SemaphoreType.DMA,
            pltpu.SemaphoreType.DMA((6,)), pltpu.SemaphoreType.DMA((2, 6)), pltpu.SemaphoreType.DMA((SLOTS + 1,)), pltpu.SemaphoreType.DMA((2,)), pltpu.SemaphoreType.DMA,
        ],
        compiler_params=pltpu.CompilerParams(collective_id=1, has_side_effects=True, vmem_limit_bytes=67043328),
        cost_estimate=pl.CostEstimate(flops=2 * 96 * 47_000_000, bytes_accessed=100_000_000, transcendentals=1_000_000),
        name="main_part",
    )(seq_lens, x_tok, g_attn.reshape(24, 128), g_mlp.reshape(24, 128), cos2, sin2, k_out, v_out, wq, wo, wg, wu, wd)


def solution(mesh):
    cache_spec = P(None, "sp", "tp", None)
    col_spec = P(None, "tp")
    row_spec = P("tp", None)
    full_spec = P()

    def local_step(x_tok, seq_lens, k_blk, v_blk, g_attn, wq_loc, wk_loc, wv_loc, wo_loc, g_mlp, wg_loc, wu_loc, wd_loc):
        k_out, v_out, cos2, sin2 = cache_part(seq_lens, x_tok, g_attn, k_blk, v_blk, wk_loc, wv_loc)
        y_out = main_part(seq_lens, x_tok, g_attn, g_mlp, cos2, sin2, k_out, v_out, wq_loc, wo_loc, wg_loc, wu_loc, wd_loc)
        return y_out, k_out.reshape(k_blk.shape), v_out.reshape(v_blk.shape)

    return jax.shard_map(local_step, mesh=mesh, in_specs=(full_spec, full_spec, cache_spec, cache_spec, full_spec, col_spec, col_spec, col_spec, row_spec, full_spec, col_spec, col_spec, row_spec), out_specs=(full_spec, cache_spec, cache_spec), check_vma=False)
```
